128 devices in a mesh: seq: 32 (over x, z, core), head: 4 (over y).
Axes of the slice: x: 4, y: 4, z: 4, core: 2. Of those that a mesh axis runs over, the one named last changes fastest.
Arguments:
- xs: bfloat16 [32768, 4096], P('seq', 'head'), may hold values from -6 to 6
- gate_branch: bfloat16 [32768, 4096], P('seq', 'head'), may hold values from -6 to 6
- bmat: bfloat16 [32768, 128], P('seq'), may hold values from -0.25 to 0.25
- cmat: bfloat16 [32768, 128], P('seq'), may hold values from -0.25 to 0.25
- dt_code: int32 [64, 32768], P('head', 'seq'), may hold values from 1 to 131072
- resets: int32 [32768], P('seq'), may hold values 0 or 1
- decay_rate: float32 [64], P('head'), may hold values from 1.2207031e-05 to 0.08, as said below
- skip: float32 [64], P('head'), may hold values from 0.5 to 1.5
- norm_gain: float32 [4096], P('head'), may hold values from 0.1 to 1.9
- out_weight: bfloat16 [4096, 4096], P('head'), may hold values from -0.09375 to 0.09375
Outputs:
- mixed: bfloat16 [32768, 4096], P(('seq', 'head'))
The draws below stay inside these ranges and needn't reach their ends.
Inputs may be any that keep to these rules, and one draw needn't show every extreme that they name: `decay_rate`: positive rates.
All inputs are finite; a program needn't handle non-finite values. No bound on the sum of `resets` on one device may be relied on, other than what follows from the above.
Results may differ from the reference program's by a relative error of at most 0.023.
Values may be sent and summed in bfloat16 or wider, within the bound.
A program may use at most 128 MiB of HBM per device.

```python
import jax
import jax.numpy as jnp
from jax import lax

D = 4096
HEADS = 64
HEAD_DIM = 64
STATE = 128
SPAN = 256
HORIZON_TICKS = 32768
INNER = 4096
GROUPS = 4


def draw_xs(key, part):
    first = jax.random.fold_in(key, 0)
    values = jax.random.normal(first, (HORIZON_TICKS, INNER), jnp.float32)
    return jnp.clip(values, -6.0, 6.0).astype(jnp.bfloat16)


def draw_dt_code(key, part):
    first, right_factor = jax.random.split(jax.random.fold_in(key, 11))
    starting_displacement = jax.random.randint(first, (HEADS, HORIZON_TICKS), 1, 17)
    contiguous_span_count = jax.random.randint(right_factor, (HORIZON_TICKS,), 0, HORIZON_TICKS) < 3
    return jnp.where(contiguous_span_count[None, :], 4 * HORIZON_TICKS, starting_displacement).astype(jnp.int32)


def draw_decay_rate(key, part):
    first, right_factor, third = jax.random.split(jax.random.fold_in(key, 23), 3)
    share = 0.5
    slow_mask = jax.random.uniform(first, (HEADS,), jnp.float32) < share
    slow_rate = jnp.exp(jax.random.uniform(right_factor, (HEADS,), jnp.float32, jnp.log(0.4), jnp.log(1.6))) / HORIZON_TICKS
    fast_rate = jnp.exp(jax.random.uniform(third, (HEADS,), jnp.float32, jnp.log(0.03), jnp.log(0.08)))
    return jnp.where(slow_mask, slow_rate, fast_rate).astype(jnp.float32)


def place_ends(drawn, key, low, high):
    longest = drawn.shape.index(max(drawn.shape))
    spots = []
    for shift in (0, 1):
        where = [jax.random.randint(jax.random.fold_in(key, axis), (), 0, length) for axis, length in enumerate(drawn.shape)]
        where[longest] = (where[longest] + shift) % drawn.shape[longest]
        spots.append(tuple(where))
    return drawn.at[spots[0]].set(low).at[spots[1]].set(high)


def shard_levels(rng, shape, shards, low, top_value):
    level, own = 1.0, jax.random.fold_in(rng, 6)
    for dim, parts in shards:
        draws = jnp.exp(jax.random.uniform(jax.random.fold_in(own, dim), (parts,), jnp.float32, low / len(shards), top_value / len(shards)))
        level = level * jnp.repeat(draws, shape[dim] // parts).reshape([-1 if axis == dim else 1 for axis in range(len(shape))])
    return level


def centred(own_key, shape, spread, reach, cuts=(), kind=jnp.bfloat16):
    entries = spread * jax.random.normal(own_key, shape, jnp.float32)
    if cuts:
        entries = entries * shard_levels(own_key, shape, cuts, -0.22, 0.18)
    return jnp.clip(entries, -reach, reach).astype(kind)


def setup_inputs(seed: int = 0) -> dict:
    key_of = jax.random.split(jax.random.key(seed), 11)
    xs = draw_xs(jax.random.fold_in(key_of[10], 71), 0)
    gate_branch = centred(key_of[1], (HORIZON_TICKS, INNER), 1.0, 6.0, ((0, 32), (1, 4)))
    bmat = centred(key_of[2], (HORIZON_TICKS, STATE), (2 * (HORIZON_TICKS * STATE) ** -0.25), 0.25, ((0, 32),))
    cmat = centred(key_of[3], (HORIZON_TICKS, STATE), (2 * (HORIZON_TICKS * STATE) ** -0.25), 0.25, ((0, 32),))
    dt_code = draw_dt_code(jax.random.fold_in(key_of[10], 71), 0)
    resets = place_ends((jax.random.randint(key_of[5], (HORIZON_TICKS,), 0, HORIZON_TICKS) < 2).astype(jnp.int32), jax.random.fold_in(key_of[5], 1), 0, 1)
    decay_rate = draw_decay_rate(jax.random.fold_in(key_of[10], 71), 0)
    skip = jnp.clip(0.5 + 1.0 * jax.random.uniform(key_of[7], (HEADS,), jnp.float32) ** shard_levels(key_of[7], (HEADS,), ((0, 4),), -0.2, 0.2), 0.5, 1.5)
    norm_gain = jnp.clip(1.0 + 0.18 * jax.random.normal(key_of[8], (INNER,), jnp.float32), 0.1, 1.9)
    out_weight = centred(key_of[9], (INNER, D), INNER ** -0.5, 0.09375, ((0, 4),))
    return {"xs": xs, "gate_branch": gate_branch, "bmat": bmat, "cmat": cmat, "dt_code": dt_code, "resets": resets, "decay_rate": decay_rate, "skip": skip, "norm_gain": norm_gain, "out_weight": out_weight}


def reference(xs, gate_branch, bmat, cmat, dt_code, resets, decay_rate, skip, norm_gain, out_weight):
    step_size = dt_code.astype(jnp.float32) / 16.0
    input_scale = jnp.minimum(step_size, 1.0)
    logarithmic_damping = -decay_rate[:, None] * step_size
    blocks = HORIZON_TICKS // SPAN
    values = xs.reshape(blocks, SPAN, HEADS, HEAD_DIM)
    key_blocks = bmat.reshape(blocks, SPAN, STATE)
    query_blocks = cmat.reshape(blocks, SPAN, STATE)
    log_blocks = logarithmic_damping.reshape(HEADS, blocks, SPAN).transpose(1, 0, 2)
    scale_blocks = input_scale.reshape(HEADS, blocks, SPAN).transpose(1, 0, 2)
    flag_blocks = resets.reshape(blocks, SPAN)

    def propagate_forward(state, inputs):
        value, key_rows, query, logs, scales, flags = inputs
        cumulative = jnp.cumsum(logs, axis=1)
        counts = jnp.cumsum(flags)
        position = jnp.arange(SPAN)
        linked = (counts[:, None] == counts[None, :]) & (position[None, :] <= position[:, None])
        gaps = jnp.where(linked[None], cumulative[:, :, None] - cumulative[:, None, :], 0.0)
        within = jnp.where(linked[None], jnp.exp(gaps), 0.0)
        intersection = jnp.dot(query, key_rows.T, preferred_element_type=jnp.float32)
        value_float = value.astype(jnp.float32)
        scaled = (value_float * scales.T[:, :, None]).astype(jnp.bfloat16)
        scaled_float = lax.optimization_barrier(scaled).astype(jnp.float32)
        scores = (within * intersection[None]).astype(jnp.bfloat16)
        scores_float = lax.optimization_barrier(scores).astype(jnp.float32)
        output = jnp.einsum('hij,jhp->ihp', scores_float, scaled_float, precision=lax.Precision.HIGHEST)
        from_start = jnp.where(counts[None, :] == 0, jnp.exp(cumulative), 0.0)
        query_float = query.astype(jnp.float32)
        carried = jnp.einsum('in,hpn->ihp', query_float, state, precision=lax.Precision.HIGHEST)
        output = output + carried * from_start.T[:, :, None]
        to_end = jnp.where(counts[None, :] == counts[-1], jnp.exp(cumulative[:, -1:] - cumulative), 0.0)
        through = jnp.where(counts[-1] == 0, jnp.exp(cumulative[:, -1]), 0.0)
        weighted = (scaled_float * to_end.T[:, :, None]).astype(jnp.bfloat16)
        weighted_float = lax.optimization_barrier(weighted).astype(jnp.float32)
        fresh = jnp.einsum('jhp,jn->hpn', weighted_float, key_rows.astype(jnp.float32), precision=lax.Precision.HIGHEST)
        state = through[:, None, None] * state + fresh
        output = output + skip[None, :, None] * value_float
        return (state, output)
    initial = jnp.zeros((HEADS, HEAD_DIM, STATE), jnp.float32)
    outputs = lax.scan(propagate_forward, initial, (values, key_blocks, query_blocks, log_blocks, scale_blocks, flag_blocks))[1]
    ssm_out = outputs.reshape(HORIZON_TICKS, INNER)
    gated = ssm_out * jax.nn.silu(gate_branch.astype(jnp.float32))
    mean_square = lax.optimization_barrier(jnp.mean(gated * gated, axis=1, keepdims=True))
    hidden = (gated * lax.rsqrt(mean_square + 1e-05) * norm_gain[None, :]).astype(jnp.bfloat16)
    group_width = INNER // GROUPS
    summed = jnp.zeros((HORIZON_TICKS, D), jnp.float32)
    for group in range(GROUPS):
        lower = group * group_width
        partial_value = jnp.dot(hidden[:, lower:lower + group_width], out_weight[lower:lower + group_width], preferred_element_type=jnp.float32).astype(jnp.bfloat16)
        summed = summed + lax.optimization_barrier(partial_value).astype(jnp.float32)
    return summed.astype(jnp.bfloat16)
```

```python
import jax
import jax.numpy as jnp
from jax import lax
from jax.experimental import pallas as pl
from jax.experimental.pallas import tpu as pltpu
from jax.sharding import PartitionSpec as P

HEAD_DIM = 64
STATE = 128
SPAN = 256
INNER = 4096
MESH = pl.DeviceIdType.MESH
LOG2E = 1.4426950408889634
F32 = jnp.float32
BF16 = jnp.bfloat16

WIDTHS = (384, 384, 512)
DIRECT = 512
DIRECT_PIECES = 4


def iota(shape, dim):
    return lax.broadcasted_iota(jnp.int32, shape, dim)


def kernel(
    xs_hbm, gate_hbm, bmat, cmat, dt, resets, gain, w_hbm, rate, skip,
    out_hbm,
    xs, gate, weight, hid, hid_send, sums, sums_send, acc, out_buf,
    tri, col, split, bt, cjp, cntrow, grow, starts, reach, chunk_send, chunk_recv, inc_send, inc_recv,
    cbm, local,
    in_sem, own_sem, slice_ss, slice_rs, direct_ss, direct_rs, step_ss, step_rs,
    chunk_ss, chunk_rs, inc_ss, inc_rs, hid_ss, hid_rs, sum_ss, sum_rs, fwd_ss, fwd_rs, fsum_ss, fsum_rs,
    out_ss, out_rs, out_sem,
):
    s = lax.axis_index("seq")
    h = lax.axis_index("head")
    x, z, c = s // 8, (s // 2) % 4, s % 2
    other = (s + 1 - 2 * c, h)

    def remote(src, dst, ss, rs, dev):
        return pltpu.make_async_remote_copy(
            src_ref=src, dst_ref=dst, send_sem=ss, recv_sem=rs, device_id=dev, device_id_type=MESH
        )

    copies_in = [
        pltpu.make_async_copy(xs_hbm, xs, in_sem.at[0]),
        pltpu.make_async_copy(gate_hbm, gate, in_sem.at[1]),
    ]
    for cp in copies_in:
        cp.start()

    barrier = pltpu.get_barrier_semaphore()

    @pl.loop(1, 32)
    def _(i):
        pl.semaphore_signal(barrier, inc=1, device_id=((s + i) % 32, h), device_id_type=MESH)

    for d in (1, 2, 3):
        pl.semaphore_signal(barrier, inc=1, device_id=(s, (h + d) % 4), device_id_type=MESH)

    planes = [(h + 1) % 4, (h + 3) % 4, (h + 2) % 4]
    arrives_as = (1, 0, 2)

    px, pz = x % 2, z % 2
    ax, az = x // 2, z // 2
    bx, bz = ((x + 1) // 2) % 2, ((z + 1) // 2) % 2
    x_a, z_a = x + 1 - 2 * px, z + 1 - 2 * pz
    x_b, z_b = (x + 3 + 2 * px) % 4, (z + 3 + 2 * pz) % 4

    def at(xx, zz):
        return ((xx * 4 + zz) * 2 + c, h)

    along = (at(x_a, z), at(x, z_a), at(x_b, z), at(x, z_b))
    bits = ((px, pz, ax, az), (pz, px, az, bx), (px, pz, bx, bz), (pz, px, bz, ax))
    mine = [b0 + 2 * b1 + 4 * b2 + 8 * b3 for b0, b1, b2, b3 in bits]
    base = c * 2048

    def slice_copy(j, k):
        rows = pl.ds(pl.multiple_of(mine[k] * 64, 64), 64)
        width = WIDTHS[arrives_as[j]]
        src = w_hbm.at[rows, pl.ds(pl.multiple_of(base + k * width, 128), width)]
        dst = weight.at[h, rows, pl.ds(k * width, width)]
        return remote(src, dst, slice_ss.at[j, k], slice_rs.at[arrives_as[j], k], (s, planes[j]))

    def slice_wait(j, k):
        rows = pl.ds(pl.multiple_of(mine[k] * 64, 64), 64)
        part = weight.at[planes[j], rows, pl.ds(k * WIDTHS[j], WIDTHS[j])]
        remote(part, part, slice_ss.at[j, k], slice_rs.at[j, k], (s, planes[j])).wait_recv()

    per = 1024 // DIRECT_PIECES

    def direct_copy(j, m):
        rows = pl.ds(m * per, per)
        src = w_hbm.at[rows, pl.ds(pl.multiple_of(base + 2048 - DIRECT, 128), DIRECT)]
        dst = weight.at[h, rows, pl.ds(2048 - DIRECT, DIRECT)]
        return remote(src, dst, direct_ss.at[j, m], direct_rs.at[1 - j, m], (s, planes[j]))

    def direct_wait(j, m):
        part = weight.at[planes[j], pl.ds(m * per, per), pl.ds(2048 - DIRECT, DIRECT)]
        remote(part, part, direct_ss.at[j, m], direct_rs.at[j, m], (s, planes[j])).wait_recv()

    def step_copy(t, j, k):
        first = (mine[k] // (1 << t)) * (64 << t)
        rows = pl.ds(pl.multiple_of(first, 64 << t), 64 << t)
        part = weight.at[planes[j], rows, pl.ds(k * WIDTHS[j], WIDTHS[j])]
        return remote(part, part, step_ss.at[t, j, k], step_rs.at[t, j, k], along[(k + t) % 4])

    own_weight = pltpu.make_async_copy(w_hbm.at[:, pl.ds(pl.multiple_of(base, 128), 2048)], weight.at[h], own_sem)
    own_weight.start()

    pl.semaphore_wait(barrier, 34)

    for j in (0, 1, 2):
        for k in range(4):
            slice_copy(j, k).start()

    tri[...] = jnp.where(iota((SPAN, SPAN), 0) <= iota((SPAN, SPAN), 1), 1.0, 0.0).astype(BF16)
    head_row = iota((16, SPAN), 0)
    slope = jnp.zeros((16, SPAN), F32)
    for n in range(16):
        slope = jnp.where(head_row == n, rate[n] * (-LOG2E / 16.0), slope)
    for b in range(4):
        d = dt[:, b * SPAN:(b + 1) * SPAN]
        flags = jnp.broadcast_to(resets[:, b * SPAN:(b + 1) * SPAN], (16, SPAN))
        parts = [d & 0xFF, d & 0xFF00, d & 0x30000, flags]
        stack = jnp.concatenate([p.astype(F32) for p in parts], axis=0).astype(BF16)
        run = jnp.dot(stack, tri[...], preferred_element_type=F32)
        c2 = (run[0:16] + run[16:32] + run[32:48]) * slope
        count = run[48:64]
        ls = jnp.log(jnp.minimum(d.astype(F32) * 0.0625, 1.0)) * LOG2E
        c2_end, count_end = c2[:, SPAN - 1:SPAN], count[:, SPAN - 1:SPAN]
        from_start = jnp.where(count == 0, jnp.exp2(c2), 0.0)
        to_end = jnp.where(count == count_end, jnp.exp2(c2_end - c2 + ls), 0.0)
        cjp[b] = c2 - ls
        cntrow[b] = count[0:8]
        table = jnp.concatenate([c2, from_start, to_end, count, jnp.zeros((64, SPAN), F32)], axis=0)
        flipped = table.T
        col[b] = flipped
        high = flipped.astype(BF16)
        low = (flipped - high.astype(F32)).astype(BF16)
        split[b] = jnp.concatenate([high, low], axis=1)
        bt[b] = bmat[b * SPAN:(b + 1) * SPAN, :].T

    copies_in[0].wait()

    @pl.loop(0, 8)
    def _(q):
        lanes = pl.ds(pl.multiple_of(q * 128, 128), 128)
        row, lane = iota((SPAN, SPAN), 0) % 128, iota((SPAN, SPAN), 1)
        pick = jnp.where(lane < 128, 16, 32) + 2 * q + (lane % 128) // 64
        pick = jnp.where(row == pick, 1.0, 0.0).astype(BF16)
        run = jnp.zeros((STATE, 128), F32)
        product = jnp.ones((1, 128), F32)
        for b in range(4):
            rows = pl.ds(b * SPAN, SPAN)
            wide = jnp.dot(split[b], pick, preferred_element_type=F32)
            grow[rows, lanes] = wide[:, 0:128]
            weighted = (xs[rows, lanes].astype(F32) * wide[:, 128:256]).astype(BF16)
            fresh = jnp.dot(bt[b], weighted, preferred_element_type=F32)
            starts[b, q] = run
            reach[b, q] = jnp.broadcast_to(product, (8, 128))
            through = wide[SPAN - 1:SPAN, 0:128]
            run = through * run + fresh
            product = product * through
        high = product.astype(BF16).astype(F32)
        rest = product - high
        mid = rest.astype(BF16).astype(F32)
        low = rest - mid
        line = iota((16, 128), 0)
        tail = jnp.where(line == 0, high, jnp.where(line == 1, mid, jnp.where(line == 2, low, 0.0))).astype(BF16)
        for r in range(4):
            chunk_send[q * 4 + r, 0:32, :] = run[r * 32:(r + 1) * 32].astype(BF16)
            chunk_send[q * 4 + r, 32:48, :] = tail

    def chunk_copy(i):
        o = (s + i) % 32
        return remote(chunk_send.at[o], chunk_recv.at[s], chunk_ss.at[i], chunk_rs.at[i], (o, h))

    @pl.loop(1, 32)
    def _(i):
        chunk_copy(i).start()

    chunk_recv[s] = chunk_send[s]

    half = SPAN // 2

    def inside(b):
        rows = pl.ds(pl.multiple_of(b * SPAN, SPAN), SPAN)
        table = col[b]
        pair = jnp.dot(cmat[rows, :], bt[b], preferred_element_type=F32)
        same = (table[:, 48:49] == cntrow[b][0:1, :]) & (iota((SPAN, SPAN), 1) <= iota((SPAN, SPAN), 0))
        cbm[...] = jnp.where(same, pair, 0.0)
        first = iota((SPAN, 128), 1) < HEAD_DIM
        for q in range(8):
            lanes = slice(q * 128, (q + 1) * 128)
            value = xs[rows, lanes]
            value_float = value.astype(F32)
            sides = (jnp.where(first, value_float, 0.0).astype(BF16), jnp.where(first, 0.0, value_float).astype(BF16))
            total = [jnp.where(first[0:half], skip[2 * q], skip[2 * q + 1]) * value_float[r * half:(r + 1) * half] for r in (0, 1)]
            for e in (0, 1):
                n = 2 * q + e
                ci = table[:, n:n + 1]
                cj = cjp[b, n:n + 1, :]
                for r in (0, 1):
                    lo, hi = r * half, (r + 1) * half
                    gap = jnp.minimum(ci[lo:hi] - cj[:, 0:hi], 0.0)
                    score = (jnp.exp2(gap) * cbm[lo:hi, 0:hi]).astype(BF16)
                    total[r] = total[r] + jnp.dot(score, sides[e][0:hi], preferred_element_type=F32)
            for r in (0, 1):
                local[pl.ds(pl.multiple_of(b * SPAN + r * half, half), half), lanes] = total[r]

    for j in (0, 1):
        for k in range(4):
            slice_wait(j, k)
            step_copy(0, j, k).start()

    pl.loop(0, 2)(inside)

    @pl.loop(1, 32)
    def _(i):
        chunk_copy(i).wait_recv()

    def scan(t, incoming):
        inc_send[t] = incoming.astype(BF16)
        tail = chunk_recv[t, 32:48, :].astype(F32)
        through = tail[0:1] + tail[1:2] + tail[2:3]
        return through * incoming + chunk_recv[t, 0:32, :].astype(F32)

    lax.fori_loop(0, 32, scan, jnp.zeros((32, 128), F32))

    def inc_copy(i):
        o = (s + i) % 32
        return remote(inc_send.at[o], inc_recv.at[s], inc_ss.at[i], inc_rs.at[i], (o, h))

    @pl.loop(1, 32)
    def _(i):
        inc_copy(i).start()

    inc_recv[s] = inc_send[s]

    for k in range(4):
        slice_wait(2, k)
        step_copy(0, 2, k).start()
    for j in (0, 1):
        for m in range(DIRECT_PIECES // 2):
            direct_copy(j, m).start()
    for j in (0, 1, 2):
        for k in range(4):
            step_copy(0, j, k).wait_recv()
            step_copy(1, j, k).start()

    pl.loop(2, 4)(inside)

    @pl.loop(1, 32)
    def _(i):
        inc_copy(i).wait_recv()

    copies_in[1].wait()

    def finish(b, put):
        rows = pl.ds(pl.multiple_of(b * SPAN, SPAN), SPAN)
        query = cmat[rows, :]

        def part(q, squares):
            lanes = pl.ds(pl.multiple_of(q * 128, 128), 128)
            incoming = inc_recv[pl.ds(q * 4, 4)].reshape(STATE, 128).astype(F32)
            state = (starts[b, q] + reach[b, q, 0:1, :] * incoming).astype(BF16)
            inter = jnp.dot(query, state, preferred_element_type=F32)
            value = local[rows, lanes] + grow[rows, lanes] * inter
            v = gate[rows, lanes].astype(F32)
            gated = value * (v / (1.0 + jnp.exp(-v)))
            put(lanes, (gated * gain[:, lanes]).astype(BF16))
            return squares + gated * gated

        squares = lax.fori_loop(0, 8, part, jnp.zeros((SPAN, 128), F32))
        total = jnp.broadcast_to(jnp.sum(squares, axis=1, keepdims=True), (SPAN, 128)).T[0:16, :]
        high = total.astype(BF16).astype(F32)
        return jnp.where(iota((16, SPAN), 0) == 0, high, total - high).astype(BF16)

    def hid_copy(j):
        there = hid.at[h, pl.ds(pl.multiple_of(c * SPAN, SPAN), SPAN), :]
        return remote(hid_send.at[j], there, hid_ss.at[j], hid_rs.at[arrives_as[j]], (s, planes[j]))

    def sum_copy(j):
        return remote(sums_send.at[j], sums.at[h, c], sum_ss.at[j], sum_rs.at[arrives_as[j]], (s, planes[j]))

    for j in (0, 1, 2):
        def put(lanes, value, j=j):
            hid_send[j, :, lanes] = value

        sums_send[j] = finish(planes[j], put)
        hid_copy(j).start()
        sum_copy(j).start()
        for k in range(4):
            step_copy(1, j, k).wait_recv()
            step_copy(2, j, k).start()

    def put_own(lanes, value):
        hid[h, pl.ds(pl.multiple_of(c * SPAN, SPAN), SPAN), lanes] = value

    sums[h, c] = finish(h, put_own)

    for j in (0, 1):
        for m in range(DIRECT_PIECES // 2, DIRECT_PIECES):
            direct_copy(j, m).start()

    def forward(n, plane):
        part = hid.at[plane, pl.ds(pl.multiple_of(c * SPAN, SPAN), SPAN), :]
        return remote(part, part, fwd_ss.at[n], fwd_rs.at[n], other)

    def forward_sums(n, plane):
        part = sums.at[plane, c]
        return remote(part, part, fsum_ss.at[n], fsum_rs.at[n], other)

    forward(3, h).start()
    forward_sums(3, h).start()

    for j in (0, 1, 2):
        for k in range(4):
            step_copy(2, j, k).wait_recv()
            step_copy(3, j, k).start()

    own_weight.wait()
    forward(3, h).wait_recv()

    @pl.loop(0, 8)
    def _(n):
        lanes = pl.ds(pl.multiple_of(n * 256, 256), 256)
        acc[:, lanes] = jnp.dot(hid[h], weight[h, :, lanes], preferred_element_type=F32)

    def wait_hid(j):
        part = hid.at[planes[j], pl.ds(pl.multiple_of(c * SPAN, SPAN), SPAN), :]
        remote(part, part, hid_ss.at[j], hid_rs.at[j], (s, planes[j])).wait_recv()
        tot = sums.at[planes[j], c]
        remote(tot, tot, sum_ss.at[j], sum_rs.at[j], (s, planes[j])).wait_recv()
        forward(j, planes[j]).start()
        forward_sums(j, planes[j]).start()

    def multiply(j, k, last):
        first = (mine[k] // 8) * 512
        if last:
            first = 512 - first
        depth = pl.ds(pl.multiple_of(first, 512), 512)
        lanes = slice(k * WIDTHS[j], (k + 1) * WIDTHS[j])
        acc[:, lanes] += jnp.dot(hid[planes[j], :, depth], weight[planes[j], depth, lanes], preferred_element_type=F32)

    for j in (0, 1, 2):
        wait_hid(j)
        forward(j, planes[j]).wait_recv()
        for k in range(4):
            multiply(j, k, False)
    for j in (0, 1):
        for m in range(DIRECT_PIECES):
            direct_wait(j, m)
        for n in range(DIRECT // 256):
            lanes = slice(2048 - DIRECT + n * 256, 2048 - DIRECT + (n + 1) * 256)
            acc[:, lanes] += jnp.dot(hid[planes[j]], weight[planes[j], :, lanes], preferred_element_type=F32)
    for j in (0, 1, 2):
        for k in range(4):
            step_copy(3, j, k).wait_recv()
            multiply(j, k, True)

    forward_sums(3, h).wait_recv()
    for j in (0, 1, 2):
        forward_sums(j, planes[j]).wait_recv()

    def scales(core):
        total = jnp.zeros((16, SPAN), F32)
        for n in range(4):
            total = total + sums[n, core].astype(F32)
        both = lax.rsqrt((total[0:1] + total[1:2]) / INNER + 1e-05)
        return jnp.broadcast_to(both, (128, SPAN)).T

    def finished(core, slot):
        factor = scales(core)
        factor = jnp.concatenate([factor, factor], axis=1)

        @pl.loop(0, 8)
        def _(n):
            lanes = pl.ds(pl.multiple_of(n * 256, 256), 256)
            rows = pl.ds(pl.multiple_of(core * SPAN, SPAN), SPAN)
            out_buf[slot, :, lanes] = (acc[rows, lanes] * factor).astype(BF16)

    columns = pl.ds(pl.multiple_of(base, 128), 2048)
    finished(1 - c, 0)
    send_out = remote(out_buf.at[0], out_hbm.at[:, columns], out_ss, out_rs, other)
    send_out.start()
    finished(c, 1)
    keep = pltpu.make_async_copy(out_buf.at[1], out_hbm.at[:, columns], out_sem)
    keep.start()

    for j in (0, 1, 2):
        for k in range(4):
            slice_copy(j, k).wait_send()
            for t in range(4):
                step_copy(t, j, k).wait_send()
        hid_copy(j).wait_send()
        sum_copy(j).wait_send()
        forward(j, planes[j]).wait_send()
        forward_sums(j, planes[j]).wait_send()
    for j in (0, 1):
        for m in range(DIRECT_PIECES):
            direct_copy(j, m).wait_send()
    forward(3, h).wait_send()
    forward_sums(3, h).wait_send()

    @pl.loop(1, 32)
    def _(i):
        chunk_copy(i).wait_send()
        inc_copy(i).wait_send()

    keep.wait()
    send_out.wait()


def local(xs, gate_branch, bmat, cmat, dt_code, resets, decay_rate, skip, norm_gain, out_weight):
    vmem = pl.BlockSpec(memory_space=pltpu.VMEM)
    hbm = pl.BlockSpec(memory_space=pl.ANY)
    smem = pl.BlockSpec(memory_space=pltpu.SMEM)
    dma = pltpu.SemaphoreType.DMA
    V = pltpu.VMEM
    return pl.pallas_call(
        kernel,
        out_shape=jax.ShapeDtypeStruct((256, 4096), BF16),
        in_specs=[hbm, hbm, vmem, vmem, vmem, vmem, vmem, hbm, smem, smem],
        out_specs=hbm,
        scratch_shapes=[
            V((1024, 1024), BF16),
            V((1024, 1024), BF16),
            V((4, 1024, 2048), BF16),
            V((4, 512, 1024), BF16),
            V((3, 256, 1024), BF16),
            V((4, 2, 16, 256), BF16),
            V((3, 16, 256), BF16),
            V((512, 2048), F32),
            V((2, 256, 2048), BF16),
            V((256, 256), BF16),
            V((4, 256, 128), F32),
            V((4, 256, 256), BF16),
            V((4, 128, 256), BF16),
            V((4, 16, 256), F32),
            V((4, 8, 256), F32),
            V((1024, 1024), F32),
            V((4, 8, 128, 128), F32),
            V((4, 8, 8, 128), F32),
            V((32, 48, 128), BF16),
            V((32, 48, 128), BF16),
            V((32, 32, 128), BF16),
            V((32, 32, 128), BF16),
            V((256, 256), F32),
            V((1024, 1024), F32),
            dma((2,)), dma, dma((3, 4)), dma((3, 4)),
            dma((2, DIRECT_PIECES)), dma((2, DIRECT_PIECES)), dma((4, 3, 4)), dma((4, 3, 4)),
            dma((32,)), dma((32,)), dma((32,)), dma((32,)),
            dma((3,)), dma((3,)), dma((3,)), dma((3,)), dma((4,)), dma((4,)), dma((4,)), dma((4,)),
            dma, dma, dma,
        ],
        compiler_params=pltpu.CompilerParams(
            collective_id=0, has_side_effects=True, vmem_limit_bytes=64 * 1024 * 1024 - 65536
        ),
    )(
        xs, gate_branch, bmat, cmat, dt_code, resets.reshape(1, 1024), norm_gain.reshape(1, 1024), out_weight,
        decay_rate, skip,
    )


def solution(mesh):
    in_specs = (
        P("seq", "head"),
        P("seq", "head"),
        P("seq", None),
        P("seq", None),
        P("head", "seq"),
        P("seq"),
        P("head"),
        P("head"),
        P("head"),
        P("head", None),
    )
    out_specs = P(("seq", "head"), None)
    return jax.shard_map(local, mesh=mesh, in_specs=in_specs, out_specs=out_specs, check_vma=False)
```

```python
import jax
import jax.numpy as jnp
from jax import lax
from jax.experimental import pallas as pl
from jax.experimental.pallas import tpu as pltpu
from jax.sharding import PartitionSpec as P

HEAD_DIM = 64
STATE = 128
SPAN = 256
INNER = 4096
MESH = pl.DeviceIdType.MESH
LOG2E = 1.4426950408889634
F32 = jnp.float32
BF16 = jnp.bfloat16

WIDTHS = (384, 384, 512)
DIRECT = 512
DIRECT_PIECES = 2


def iota(shape, dim):
    return lax.broadcasted_iota(jnp.int32, shape, dim)


def kernel(
    xs_hbm, gate_hbm, bmat, cmat, dt, resets, gain, w_hbm, rate, skip,
    out,
    xs, gate, weight, hid, hid_send, sums, sums_send, acc, out_send,
    tri, col, split, bt, cjp, cntrow, grow, starts, reach, whole_send, pair_recv, chunk_send, chunk_recv, inc_send, inc_recv,
    pair_out, incoming, cbm, local,
    in_sem, own_sem, slice_ss, slice_rs, direct_ss, direct_rs, step_ss, step_rs,
    pair_ss, pair_rs, chunk_ss, chunk_rs, inc_ss, inc_rs, last_ss, last_rs, hid_ss, hid_rs, sum_ss, sum_rs, fwd_ss, fwd_rs, fsum_ss, fsum_rs,
    out_ss, out_rs,
):
    s = lax.axis_index("seq")
    h = lax.axis_index("head")
    x, z, c = s // 8, (s // 2) % 4, s % 2
    other = (s + 1 - 2 * c, h)

    def remote(src, dst, ss, rs, dev):
        return pltpu.make_async_remote_copy(
            src_ref=src, dst_ref=dst, send_sem=ss, recv_sem=rs, device_id=dev, device_id_type=MESH
        )

    copies_in = [
        pltpu.make_async_copy(xs_hbm, xs, in_sem.at[0]),
        pltpu.make_async_copy(gate_hbm, gate, in_sem.at[1]),
    ]
    for cp in copies_in:
        cp.start()

    barrier = pltpu.get_barrier_semaphore()
    chip = s // 2

    def same_core(i):
        return ((chip + i) % 16 * 2 + c, h)

    @pl.loop(1, 16)
    def _(i):
        pl.semaphore_signal(barrier, inc=1, device_id=same_core(i), device_id_type=MESH)

    pl.semaphore_signal(barrier, inc=1, device_id=other, device_id_type=MESH)
    for d in (1, 2, 3):
        pl.semaphore_signal(barrier, inc=1, device_id=(s, (h + d) % 4), device_id_type=MESH)

    planes = [(h + 1) % 4, (h + 3) % 4, (h + 2) % 4]
    arrives_as = (1, 0, 2)

    px, pz = x % 2, z % 2
    ax, az = x // 2, z // 2
    bx, bz = ((x + 1) // 2) % 2, ((z + 1) // 2) % 2
    x_a, z_a = x + 1 - 2 * px, z + 1 - 2 * pz
    x_b, z_b = (x + 3 + 2 * px) % 4, (z + 3 + 2 * pz) % 4

    def at(xx, zz):
        return ((xx * 4 + zz) * 2 + c, h)

    along = (at(x_a, z), at(x, z_a), at(x_b, z), at(x, z_b))
    bits = ((px, pz, ax, az), (pz, px, az, bx), (px, pz, bx, bz), (pz, px, bz, ax))
    mine = [b0 + 2 * b1 + 4 * b2 + 8 * b3 for b0, b1, b2, b3 in bits]
    base = c * 2048

    def slice_copy(j, k):
        rows = pl.ds(pl.multiple_of(mine[k] * 64, 64), 64)
        width = WIDTHS[arrives_as[j]]
        src = w_hbm.at[rows, pl.ds(pl.multiple_of(base + k * width, 128), width)]
        dst = weight.at[h, rows, pl.ds(k * width, width)]
        return remote(src, dst, slice_ss.at[j], slice_rs.at[arrives_as[j]], (s, planes[j]))

    def slice_all(j):
        part = weight.at[planes[j], pl.ds(0, 64), pl.ds(0, 4 * WIDTHS[j])]
        return remote(part, part, slice_ss.at[arrives_as[j]], slice_rs.at[j], (s, planes[j]))

    per = 1024 // DIRECT_PIECES

    def direct_copy(j, m):
        rows = pl.ds(m * per, per)
        src = w_hbm.at[rows, pl.ds(pl.multiple_of(base + 2048 - DIRECT, 128), DIRECT)]
        dst = weight.at[h, rows, pl.ds(2048 - DIRECT, DIRECT)]
        return remote(src, dst, direct_ss.at[j, m], direct_rs.at[1 - j, m], (s, planes[j]))

    def direct_wait(j, m):
        part = weight.at[planes[j], pl.ds(m * per, per), pl.ds(2048 - DIRECT, DIRECT)]
        remote(part, part, direct_ss.at[j, m], direct_rs.at[j, m], (s, planes[j])).wait_recv()

    def step_parts(t, j):
        return 2 if (t, j) == (3, 2) else 1

    def step_copy(t, j, k, n):
        size = (64 << t) // step_parts(t, j)
        first = (mine[k] // (1 << t)) * (64 << t) + n * size
        rows = pl.ds(pl.multiple_of(first, size), size)
        part = weight.at[planes[j], rows, pl.ds(k * WIDTHS[j], WIDTHS[j])]
        return remote(part, part, step_ss.at[t, j + n], step_rs.at[t, j + n], along[(k + t) % 4])

    def step_all(t, j, n=0):
        part = weight.at[planes[j], pl.ds(0, (64 << t) // step_parts(t, j)), pl.ds(0, 4 * WIDTHS[j])]
        return remote(part, part, step_ss.at[t, j + n], step_rs.at[t, j + n], other)

    def step_send(t, j):
        for n in range(step_parts(t, j)):
            for k in range(4):
                step_copy(t, j, k, n).start()

    def relay(t, j):
        if t == 0:
            slice_all(j).wait_recv()
        else:
            step_all(t - 1, j).wait_recv()
        step_send(t, j)

    own_weight = pltpu.make_async_copy(w_hbm.at[:, pl.ds(pl.multiple_of(base, 128), 2048)], weight.at[h], own_sem)
    own_weight.start()

    tri[...] = jnp.where(iota((SPAN, SPAN), 0) <= iota((SPAN, SPAN), 1), 1.0, 0.0).astype(BF16)
    head_row = iota((16, SPAN), 0)
    slope = jnp.zeros((16, SPAN), F32)
    for n in range(16):
        slope = jnp.where(head_row == n, rate[n] * (-LOG2E / 16.0), slope)
    for b in range(4):
        d = dt[:, b * SPAN:(b + 1) * SPAN]
        flags = jnp.broadcast_to(resets[:, b * SPAN:(b + 1) * SPAN], (16, SPAN))
        parts = [d & 0xFF, d & 0xFF00, d & 0x30000, flags]
        stack = jnp.concatenate([p.astype(F32) for p in parts], axis=0).astype(BF16)
        run = jnp.dot(stack, tri[...], preferred_element_type=F32)
        c2 = (run[0:16] + run[16:32] + run[32:48]) * slope
        count = run[48:64]
        ls = jnp.log(jnp.minimum(d.astype(F32) * 0.0625, 1.0)) * LOG2E
        c2_end, count_end = c2[:, SPAN - 1:SPAN], count[:, SPAN - 1:SPAN]
        from_start = jnp.where(count == 0, jnp.exp2(c2), 0.0)
        to_end = jnp.where(count == count_end, jnp.exp2(c2_end - c2 + ls), 0.0)
        cjp[b] = c2 - ls
        cntrow[b] = count[0:8]
        table = jnp.concatenate([c2, from_start, to_end, count, jnp.zeros((64, SPAN), F32)], axis=0)
        flipped = table.T
        col[b] = flipped
        high = flipped.astype(BF16)
        low = (flipped - high.astype(F32)).astype(BF16)
        split[b] = jnp.concatenate([high, low], axis=1)
        bt[b] = bmat[b * SPAN:(b + 1) * SPAN, :].T

    pl.semaphore_wait(barrier, 19)

    for j in (0, 1):
        for k in range(4):
            slice_copy(j, k).start()

    copies_in[0].wait()

    def in_parts(row):
        high = row.astype(BF16).astype(F32)
        mid = (row - high).astype(BF16).astype(F32)
        line = iota((16, 128), 0)
        low = row - high - mid
        return jnp.where(line == 0, high, jnp.where(line == 1, mid, jnp.where(line == 2, low, 0.0))).astype(BF16)

    def from_parts(rows):
        rows = rows.astype(F32)
        return rows[0:1] + rows[1:2] + rows[2:3]

    def states(group):
        row, lane = iota((SPAN, SPAN), 0) % 128, iota((SPAN, SPAN), 1)
        wides, fresh = {}, {}
        for q in group:
            pick = jnp.where(lane < 128, 16, 32) + 2 * q + (lane % 128) // 64
            pick = jnp.where(row == pick, 1.0, 0.0).astype(BF16)
            for b in range(4):
                wides[q, b] = jnp.dot(split[b], pick, preferred_element_type=F32)
        for q in group:
            lanes = slice(q * 128, (q + 1) * 128)
            for b in range(4):
                rows = slice(b * SPAN, (b + 1) * SPAN)
                grow[rows, lanes] = wides[q, b][:, 0:128]
                weighted = (xs[rows, lanes].astype(F32) * wides[q, b][:, 128:256]).astype(BF16)
                fresh[q, b] = jnp.dot(bt[b], weighted, preferred_element_type=F32)
        for q in group:
            run = jnp.zeros((STATE, 128), F32)
            product = jnp.ones((1, 128), F32)
            for b in range(4):
                starts[b, q] = run
                reach[b, q] = jnp.broadcast_to(product, (8, 128))
                through = wides[q, b][SPAN - 1:SPAN, 0:128]
                run = through * run + fresh[q, b]
                product = product * through
            whole_send[q, 0:128, :] = run.astype(BF16)
            whole_send[q, 128:144, :] = in_parts(product)

    for q in range(0, 8, 2):
        states((q, q + 1))

    theirs = whole_send.at[pl.ds(4 - 4 * c, 4)]
    pair = remote(theirs, pair_recv, pair_ss, pair_rs, other)
    pair.start()

    half = SPAN // 2

    def inside(b):
        rows = pl.ds(pl.multiple_of(b * SPAN, SPAN), SPAN)
        table = col[b]
        pair = jnp.dot(cmat[rows, :], bt[b], preferred_element_type=F32)
        same = (table[:, 48:49] == cntrow[b][0:1, :]) & (iota((SPAN, SPAN), 1) <= iota((SPAN, SPAN), 0))
        cbm[...] = jnp.where(same, pair, 0.0)
        first = iota((SPAN, 128), 1) < HEAD_DIM
        for q in range(8):
            lanes = slice(q * 128, (q + 1) * 128)
            value = xs[rows, lanes]
            value_float = value.astype(F32)
            sides = (jnp.where(first, value_float, 0.0).astype(BF16), jnp.where(first, 0.0, value_float).astype(BF16))
            total = [jnp.where(first[0:half], skip[2 * q], skip[2 * q + 1]) * value_float[r * half:(r + 1) * half] for r in (0, 1)]
            for e in (0, 1):
                n = 2 * q + e
                ci = table[:, n:n + 1]
                cj = cjp[b, n:n + 1, :]
                for r in (0, 1):
                    lo, hi = r * half, (r + 1) * half
                    gap = jnp.minimum(ci[lo:hi] - cj[:, 0:hi], 0.0)
                    score = (jnp.exp2(gap) * cbm[lo:hi, 0:hi]).astype(BF16)
                    total[r] = total[r] + jnp.dot(score, sides[e][0:hi], preferred_element_type=F32)
            for r in (0, 1):
                local[pl.ds(pl.multiple_of(b * SPAN + r * half, half), half), lanes] = total[r]

    inside(0)

    pair.wait_recv()
    first_core = c == 0
    for n in range(4):
        own, far = whole_send[4 * c + n], pair_recv[n]
        own_through, far_through = from_parts(own[128:144]), from_parts(far[128:144])
        own_state, far_state = own[0:128].astype(F32), far[0:128].astype(F32)
        earlier = jnp.where(first_core, own_state, far_state)
        later = jnp.where(first_core, far_state, own_state)
        total = jnp.where(first_core, far_through, own_through) * earlier + later
        tail = in_parts(own_through * far_through)
        for r in range(4):
            chunk_send[n * 4 + r, 0:32, :] = total[r * 32:(r + 1) * 32].astype(BF16)
            chunk_send[n * 4 + r, 32:48, :] = tail

    @pl.loop(1, 16)
    def _(i):
        remote(chunk_send.at[(chip + i) % 16], chunk_recv.at[chip], chunk_ss, chunk_rs, same_core(i)).start()

    chunk_recv[chip] = chunk_send[chip]

    for k in range(4):
        slice_copy(2, k).start()
    inside(1)
    inside(2)
    for j in (0, 1):
        direct_copy(j, 0).start()

    relay(0, 0)
    relay(0, 1)

    arrived = chunk_recv.at[pl.ds(0, 15)]
    chunk_all = remote(arrived, arrived, chunk_ss, chunk_rs, other)
    chunk_all.wait_recv()

    state = jnp.zeros((32, 128), F32)
    for t in range(16):
        inc_send[t] = state.astype(BF16)
        state = from_parts(chunk_recv[t, 32:48, :]) * state + chunk_recv[t, 0:32, :].astype(F32)

    @pl.loop(1, 16)
    def _(i):
        remote(inc_send.at[(chip + i) % 16], inc_recv.at[chip], inc_ss, inc_rs, same_core(i)).start()

    inc_recv[chip] = inc_send[chip]

    inside(3)
    relay(1, 0)
    relay(1, 1)
    relay(0, 2)

    returned = inc_recv.at[pl.ds(0, 15)]
    inc_all = remote(returned, returned, inc_ss, inc_rs, other)
    inc_all.wait_recv()
    for n in range(4):
        own, far = whole_send[4 * c + n], pair_recv[n]
        first_state = jnp.where(first_core, own[0:128].astype(F32), far[0:128].astype(F32))
        first_through = jnp.where(first_core, from_parts(own[128:144]), from_parts(far[128:144]))
        reaching = inc_recv[n * 4:(n + 1) * 4].reshape(STATE, 128)
        second = (first_through * reaching.astype(F32) + first_state).astype(BF16)
        incoming[4 * c + n] = jnp.where(first_core, reaching.astype(F32), second.astype(F32)).astype(BF16)
        pair_out[n] = jnp.where(first_core, second.astype(F32), reaching.astype(F32)).astype(BF16)
    handed = remote(pair_out, incoming.at[pl.ds(4 * c, 4)], last_ss, last_rs, other)
    handed.start()
    relay(2, 0)
    relay(2, 1)
    handed.wait_recv()
    copies_in[1].wait()

    def finish(b, put):
        rows = pl.ds(pl.multiple_of(b * SPAN, SPAN), SPAN)
        query = cmat[rows, :]

        def part(q, squares):
            lanes = pl.ds(pl.multiple_of(q * 128, 128), 128)
            state = (starts[b, q] + reach[b, q, 0:1, :] * incoming[q].astype(F32)).astype(BF16)
            inter = jnp.dot(query, state, preferred_element_type=F32)
            value = local[rows, lanes] + grow[rows, lanes] * inter
            v = gate[rows, lanes].astype(F32)
            gated = value * (v / (1.0 + jnp.exp(-v)))
            put(lanes, (gated * gain[:, lanes]).astype(BF16))
            return squares + gated * gated

        squares = lax.fori_loop(0, 8, part, jnp.zeros((SPAN, 128), F32))
        total = jnp.broadcast_to(jnp.sum(squares, axis=1, keepdims=True), (SPAN, 128)).T[0:16, :]
        high = total.astype(BF16).astype(F32)
        return jnp.where(iota((16, SPAN), 0) == 0, high, total - high).astype(BF16)

    def hid_copy(j):
        there = hid.at[h, pl.ds(pl.multiple_of(c * SPAN, SPAN), SPAN), :]
        return remote(hid_send.at[j], there, hid_ss.at[j], hid_rs.at[arrives_as[j]], (s, planes[j]))

    def sum_copy(j):
        return remote(sums_send.at[j], sums.at[c, h], sum_ss, sum_rs, (s, planes[j]))

    for j in (0, 1, 2):
        def put(lanes, value, j=j):
            hid_send[j, :, lanes] = value

        sums_send[j] = finish(planes[j], put)
        hid_copy(j).start()
        sum_copy(j).start()
        if j == 0:
            relay(1, 2)

    def put_own(lanes, value):
        hid[h, pl.ds(pl.multiple_of(c * SPAN, SPAN), SPAN), lanes] = value

    sums[c, h] = finish(h, put_own)

    for j in (0, 1):
        direct_copy(j, 1).start()

    def forward(n, plane):
        part = hid.at[plane, pl.ds(pl.multiple_of(c * SPAN, SPAN), SPAN), :]
        return remote(part, part, fwd_ss.at[n], fwd_rs.at[n], other)

    forward(3, h).start()

    relay(3, 0)
    relay(2, 2)
    relay(3, 1)

    own_weight.wait()
    forward(3, h).wait_recv()

    @pl.loop(0, 8)
    def _(n):
        lanes = pl.ds(pl.multiple_of(n * 256, 256), 256)
        acc[:, lanes] = jnp.dot(hid[h], weight[h, :, lanes], preferred_element_type=F32)

    relay(3, 2)

    def wait_hid(j):
        part = hid.at[planes[j], pl.ds(pl.multiple_of(c * SPAN, SPAN), SPAN), :]
        remote(part, part, hid_ss.at[j], hid_rs.at[j], (s, planes[j])).wait_recv()
        forward(j, planes[j]).start()

    def depth_of(k, last, n, parts):
        first = (mine[k] // 8) * 512
        if last:
            first = 512 - first
        size = 512 // parts
        return pl.ds(pl.multiple_of(first + n * size, size), size)

    def multiply(j, k, last, n=0, parts=1):
        depth = depth_of(k, last, n, parts)
        lanes = slice(k * WIDTHS[j], (k + 1) * WIDTHS[j])
        acc[:, lanes] += jnp.dot(hid[planes[j], :, depth], weight[planes[j], depth, lanes], preferred_element_type=F32)

    for j in (0, 1, 2):
        wait_hid(j)
    totals = sums.at[c, pl.ds(0, 3)]
    remote(totals, totals, sum_ss, sum_rs, other).wait_recv()
    forward_sums = remote(sums.at[c], sums.at[c], fsum_ss, fsum_rs, other)
    forward_sums.start()
    for j in (0, 1, 2):
        forward(j, planes[j]).wait_recv()
        for k in range(4):
            multiply(j, k, False)

    forward_sums.wait_recv()

    def scales(core):
        total = jnp.zeros((16, SPAN), F32)
        for n in range(4):
            total = total + sums[core, n].astype(F32)
        both = lax.rsqrt((total[0:1] + total[1:2]) / INNER + 1e-05)
        return jnp.broadcast_to(both, (128, SPAN)).T

    factors = [scales(core) for core in (1 - c, c)]

    for j in (0, 1):
        for m in range(DIRECT_PIECES):
            direct_wait(j, m)
        for n in range(DIRECT // 256):
            lanes = slice(2048 - DIRECT + n * 256, 2048 - DIRECT + (n + 1) * 256)
            acc[:, lanes] += jnp.dot(hid[planes[j]], weight[planes[j], :, lanes], preferred_element_type=F32)
    for j in (0, 1):
        step_all(3, j).wait_recv()
        for k in range(4):
            multiply(j, k, True)
    step_all(3, 2, 0).wait_recv()
    for k in range(4):
        multiply(2, k, True, 0, 2)
    step_all(3, 2, 1).wait_recv()

    out_copies = []
    for turn, core in enumerate((1 - c, c)):
        rows = pl.ds(pl.multiple_of(core * SPAN, SPAN), SPAN)
        factor = jnp.concatenate([factors[turn]] * 4, axis=1)
        for k in range(4):
            depth = depth_of(k, True, 1, 2)
            lanes = slice(k * 512, (k + 1) * 512)
            columns = pl.ds(pl.multiple_of(c * 2048 + k * 512, 512), 512)
            last = jnp.dot(hid[planes[2], rows, depth], weight[planes[2], depth, lanes], preferred_element_type=F32)
            value = ((acc[rows, lanes] + last) * factor).astype(BF16)
            if turn == 0:
                out_send[:, lanes] = value
                copy = remote(out_send.at[:, lanes], out.at[:, columns], out_ss, out_rs, other)
                copy.start()
            else:
                out[:, columns] = value

    for j in (0, 1, 2):
        slice_all(j).wait_send()
        for t in range(4):
            for n in range(step_parts(t, j)):
                step_all(t, j, n).wait_send()
        hid_copy(j).wait_send()
        forward(j, planes[j]).wait_send()
    totals_sent = remote(sums_send, sums_send, sum_ss, sum_rs, other)
    totals_sent.wait_send()
    for j in (0, 1):
        for m in range(DIRECT_PIECES):
            direct_copy(j, m).wait_send()
    forward(3, h).wait_send()
    forward_sums.wait_send()
    pair.wait_send()
    chunk_all.wait_send()
    inc_all.wait_send()
    handed.wait_send()
    whole = remote(out_send, out_send, out_ss, out_rs, other)
    whole.wait_send()
    whole.wait_recv()


def local(xs, gate_branch, bmat, cmat, dt_code, resets, decay_rate, skip, norm_gain, out_weight):
    vmem = pl.BlockSpec(memory_space=pltpu.VMEM)
    hbm = pl.BlockSpec(memory_space=pl.ANY)
    smem = pl.BlockSpec(memory_space=pltpu.SMEM)
    dma = pltpu.SemaphoreType.DMA
    V = pltpu.VMEM
    return pl.pallas_call(
        kernel,
        out_shape=pltpu.VMEM((256, 4096), BF16),
        in_specs=[hbm, hbm, vmem, vmem, vmem, vmem, vmem, hbm, smem, smem],
        out_specs=vmem,
        scratch_shapes=[
            V((1024, 1024), BF16),
            V((1024, 1024), BF16),
            V((4, 1024, 2048), BF16),
            V((4, 512, 1024), BF16),
            V((3, 256, 1024), BF16),
            V((2, 4, 16, 256), BF16),
            V((3, 16, 256), BF16),
            V((512, 2048), F32),
            V((256, 2048), BF16),
            V((256, 256), BF16),
            V((4, 256, 128), F32),
            V((4, 256, 256), BF16),
            V((4, 128, 256), BF16),
            V((4, 16, 256), F32),
            V((4, 8, 256), F32),
            V((1024, 1024), F32),
            V((4, 8, 128, 128), F32),
            V((4, 8, 8, 128), F32),
            V((8, 144, 128), BF16),
            V((4, 144, 128), BF16),
            V((16, 48, 128), BF16),
            V((16, 48, 128), BF16),
            V((16, 32, 128), BF16),
            V((16, 32, 128), BF16),
            V((4, 128, 128), BF16),
            V((8, 128, 128), BF16),
            V((256, 256), F32),
            V((1024, 1024), F32),
            dma((2,)), dma, dma((3,)), dma((3,)),
            dma((2, DIRECT_PIECES)), dma((2, DIRECT_PIECES)), dma((4, 4)), dma((4, 4)),
            dma, dma, dma, dma, dma, dma, dma, dma,
            dma((3,)), dma((3,)), dma, dma, dma((4,)), dma((4,)), dma, dma,
            dma, dma,
        ],
        compiler_params=pltpu.CompilerParams(
            collective_id=0, has_side_effects=True, vmem_limit_bytes=58 * 1024 * 1024
        ),
    )(
        xs, gate_branch, bmat, cmat, dt_code, resets.reshape(1, 1024), norm_gain.reshape(1, 1024), out_weight,
        decay_rate, skip,
    )


def solution(mesh):
    in_specs = (
        P("seq", "head"),
        P("seq", "head"),
        P("seq", None),
        P("seq", None),
        P("head", "seq"),
        P("seq"),
        P("head"),
        P("head"),
        P("head"),
        P("head", None),
    )
    out_specs = P(("seq", "head"), None)
    return jax.shard_map(local, mesh=mesh, in_specs=in_specs, out_specs=out_specs, check_vma=False)
```

```python
import jax
import jax.numpy as jnp
from jax import lax
from jax.experimental import pallas as pl
from jax.experimental.pallas import tpu as pltpu
from jax.sharding import PartitionSpec as P

HEAD_DIM = 64
STATE = 128
SPAN = 256
INNER = 4096
MESH = pl.DeviceIdType.MESH
LOG2E = 1.4426950408889634
F32 = jnp.float32
BF16 = jnp.bfloat16

COLOURS = (
    ((0, 384), (384, 256), (640, 384), (1024, 256)),
    ((0, 256), (256, 384), (640, 256), (896, 384)),
    ((0, 512), (512, 512), (1024, 512), (1536, 512)),
)
DIRECT = slice(1280, 1536)
DIRECT_PIECES = 2
PRODUCT = slice(1536, 2048)
LAST = ((0, 256), (256, 128), (384, 128))


def iota(shape, dim):
    return lax.broadcasted_iota(jnp.int32, shape, dim)


def kernel(
    xs_hbm, gate_hbm, bmat_hbm, cmat_hbm, dt_hbm, resets_hbm, gain_hbm, w_hbm, rate, skip,
    out,
    xs, gate, bmat, cmat, dt, resets, gain, weight, hid, hid_send, hid_far, product_send, product_recv, sums, sums_send, acc, done,
    tri, col, split, bt, cjp, cntrow, grow, starts, reach, whole_send, pair_recv, chunk_send, chunk_recv, inc_send, inc_recv,
    pair_out, incoming, cbm, local,
    in_sem, own_sem, slice_ss, slice_rs, direct_ss, direct_rs, far_ss, far_rs, product_ss, product_rs, step_ss, step_rs,
    pair_ss, pair_rs, chunk_ss, chunk_rs, inc_ss, inc_rs, last_ss, last_rs, hid_ss, hid_rs, sum_ss, sum_rs, fwd_ss, fwd_rs, fsum_ss, fsum_rs,
    out_ss, out_rs,
):
    s = lax.axis_index("seq")
    h = lax.axis_index("head")
    x, z, c = s // 8, (s // 2) % 4, s % 2
    other = (s + 1 - 2 * c, h)

    def remote(src, dst, ss, rs, dev):
        return pltpu.make_async_remote_copy(
            src_ref=src, dst_ref=dst, send_sem=ss, recv_sem=rs, device_id=dev, device_id_type=MESH
        )

    barrier = pltpu.get_barrier_semaphore()
    chip = s // 2

    def same_core(i):
        return ((chip + i) % 16 * 2 + c, h)

    @pl.loop(1, 16)
    def _(i):
        pl.semaphore_signal(barrier, inc=1, device_id=same_core(i), device_id_type=MESH)

    pl.semaphore_signal(barrier, inc=1, device_id=other, device_id_type=MESH)
    for d in (1, 2, 3):
        pl.semaphore_signal(barrier, inc=1, device_id=(s, (h + d) % 4), device_id_type=MESH)

    sources = (dt_hbm, resets_hbm, bmat_hbm, cmat_hbm, xs_hbm, gate_hbm, gain_hbm)
    places = (dt, resets, bmat, cmat, xs, gate, gain)
    copies_in = [pltpu.make_async_copy(a, b, in_sem.at[n]) for n, (a, b) in enumerate(zip(sources, places))]
    for cp in copies_in:
        cp.start()

    planes = [(h + 1) % 4, (h + 3) % 4, (h + 2) % 4]
    arrives_as = (1, 0, 2)

    px, pz = x % 2, z % 2
    ax, az = x // 2, z // 2
    bx, bz = ((x + 1) // 2) % 2, ((z + 1) // 2) % 2
    x_a, z_a = x + 1 - 2 * px, z + 1 - 2 * pz
    x_b, z_b = (x + 3 + 2 * px) % 4, (z + 3 + 2 * pz) % 4

    def at(xx, zz):
        return ((xx * 4 + zz) * 2 + c, h)

    along = (at(x_a, z), at(x, z_a), at(x_b, z), at(x, z_b))
    bits = ((px, pz, ax, az), (pz, px, az, bx), (px, pz, bx, bz), (pz, px, bz, ax))
    mine = [b0 + 2 * b1 + 4 * b2 + 8 * b3 for b0, b1, b2, b3 in bits]
    base = c * 2048

    def slice_send(j):
        for k in range(4):
            first, width = COLOURS[arrives_as[j]][k]
            rows = pl.ds(pl.multiple_of(mine[k] * 64, 64), 64)
            src = w_hbm.at[rows, pl.ds(pl.multiple_of(base + first, 128), width)]
            dst = weight.at[h, rows, pl.ds(first, width)]
            remote(src, dst, slice_ss.at[j], slice_rs.at[arrives_as[j]], (s, planes[j])).start()

    def amount(t, j):
        return weight.at[planes[j], pl.ds(0, 64 << t), pl.ds(0, 2048 if j == 2 else 1280)]

    def slice_all(j):
        part = amount(0, j)
        return remote(part, part, slice_ss.at[arrives_as[j]], slice_rs.at[j], (s, planes[j]))

    per = 1024 // DIRECT_PIECES

    def direct_copy(j, m):
        rows = pl.ds(m * per, per)
        src = w_hbm.at[rows, pl.ds(pl.multiple_of(base + 1280, 128), 256)]
        dst = weight.at[h, rows, pl.ds(1280, 256)]
        return remote(src, dst, direct_ss.at[j, m], direct_rs.at[1 - j, m], (s, planes[j]))

    def direct_wait(j, m):
        part = weight.at[planes[j], pl.ds(m * per, per), pl.ds(1280, 256)]
        remote(part, part, direct_ss.at[j, m], direct_rs.at[j, m], (s, planes[j])).wait_recv()

    def step_parts(t, j):
        return len(LAST) if (t, j) == (3, 2) else 1

    def step_all(t, j, n=0):
        part = amount(t, j)
        if (t, j) == (3, 2):
            part = weight.at[planes[j], pl.ds(0, 512), pl.ds(0, 4 * LAST[n][1])]
        return remote(part, part, step_ss.at[t, j + n], step_rs.at[t, j + n], other)

    def step_send(t, j):
        for n in range(step_parts(t, j)):
            for k in range(4):
                column, width = COLOURS[j][k]
                if (t, j) == (3, 2):
                    column, width = column + LAST[n][0], LAST[n][1]
                first = (mine[k] // (1 << t)) * (64 << t)
                rows = pl.ds(pl.multiple_of(first, 64 << t), 64 << t)
                part = weight.at[planes[j], rows, pl.ds(column, width)]
                remote(part, part, step_ss.at[t, j + n], step_rs.at[t, j + n], along[(k + t) % 4]).start()

    def relay(t, j):
        if t == 0:
            slice_all(j).wait_recv()
        else:
            step_all(t - 1, j).wait_recv()
        step_send(t, j)

    own_weight = pltpu.make_async_copy(w_hbm.at[:, pl.ds(pl.multiple_of(base, 128), 2048)], weight.at[h], own_sem)
    own_weight.start()

    pl.semaphore_wait(barrier, 19)

    slice_send(0)
    slice_send(1)

    tri[...] = jnp.where(iota((SPAN, SPAN), 0) <= iota((SPAN, SPAN), 1), 1.0, 0.0).astype(BF16)
    for n in (0, 1, 2):
        copies_in[n].wait()
    head_row = iota((16, SPAN), 0)
    slope = jnp.zeros((16, SPAN), F32)
    for n in range(16):
        slope = jnp.where(head_row == n, rate[n] * (-LOG2E / 16.0), slope)
    for b in range(4):
        d = dt[:, b * SPAN:(b + 1) * SPAN]
        flags = jnp.broadcast_to(resets[:, b * SPAN:(b + 1) * SPAN], (16, SPAN))
        parts = [d & 0xFF, d & 0xFF00, d & 0x30000, flags]
        stack = jnp.concatenate([p.astype(F32) for p in parts], axis=0).astype(BF16)
        run = jnp.dot(stack, tri[...], preferred_element_type=F32)
        c2 = (run[0:16] + run[16:32] + run[32:48]) * slope
        count = run[48:64]
        ls = jnp.log(jnp.minimum(d.astype(F32) * 0.0625, 1.0)) * LOG2E
        c2_end, count_end = c2[:, SPAN - 1:SPAN], count[:, SPAN - 1:SPAN]
        from_start = jnp.where(count == 0, jnp.exp2(c2), 0.0)
        to_end = jnp.where(count == count_end, jnp.exp2(c2_end - c2 + ls), 0.0)
        cjp[b] = c2 - ls
        cntrow[b] = count[0:8]
        table = jnp.concatenate([c2, from_start, to_end, count, jnp.zeros((64, SPAN), F32)], axis=0)
        flipped = table.T
        col[b] = flipped
        high = flipped.astype(BF16)
        low = (flipped - high.astype(F32)).astype(BF16)
        split[b] = jnp.concatenate([high, low], axis=1)
        bt[b] = bmat[b * SPAN:(b + 1) * SPAN, :].T

    copies_in[3].wait()
    copies_in[4].wait()

    def in_parts(row):
        high = row.astype(BF16).astype(F32)
        mid = (row - high).astype(BF16).astype(F32)
        line = iota((16, 128), 0)
        low = row - high - mid
        return jnp.where(line == 0, high, jnp.where(line == 1, mid, jnp.where(line == 2, low, 0.0))).astype(BF16)

    def from_parts(rows):
        rows = rows.astype(F32)
        return rows[0:1] + rows[1:2] + rows[2:3]

    def states(group):
        row, lane = iota((SPAN, SPAN), 0) % 128, iota((SPAN, SPAN), 1)
        wides, fresh = {}, {}
        for q in group:
            pick = jnp.where(lane < 128, 16, 32) + 2 * q + (lane % 128) // 64
            pick = jnp.where(row == pick, 1.0, 0.0).astype(BF16)
            for b in range(4):
                wides[q, b] = jnp.dot(split[b], pick, preferred_element_type=F32)
        for q in group:
            lanes = slice(q * 128, (q + 1) * 128)
            for b in range(4):
                rows = slice(b * SPAN, (b + 1) * SPAN)
                grow[rows, lanes] = wides[q, b][:, 0:128]
                weighted = (xs[rows, lanes].astype(F32) * wides[q, b][:, 128:256]).astype(BF16)
                fresh[q, b] = jnp.dot(bt[b], weighted, preferred_element_type=F32)
        for q in group:
            run = jnp.zeros((STATE, 128), F32)
            product = jnp.ones((1, 128), F32)
            for b in range(4):
                starts[b, q] = run
                reach[b, q] = jnp.broadcast_to(product, (8, 128))
                through = wides[q, b][SPAN - 1:SPAN, 0:128]
                run = through * run + fresh[q, b]
                product = product * through
            whole_send[q, 0:128, :] = run.astype(BF16)
            whole_send[q, 128:144, :] = in_parts(product)

    for q in range(0, 8, 2):
        states((q, q + 1))

    theirs = whole_send.at[pl.ds(4 - 4 * c, 4)]
    pair = remote(theirs, pair_recv, pair_ss, pair_rs, other)
    pair.start()

    half = SPAN // 2

    def inside(b):
        rows = pl.ds(pl.multiple_of(b * SPAN, SPAN), SPAN)
        table = col[b]
        pair = jnp.dot(cmat[rows, :], bt[b], preferred_element_type=F32)
        same = (table[:, 48:49] == cntrow[b][0:1, :]) & (iota((SPAN, SPAN), 1) <= iota((SPAN, SPAN), 0))
        cbm[...] = jnp.where(same, pair, 0.0)
        first = iota((SPAN, 128), 1) < HEAD_DIM
        for q in range(8):
            lanes = slice(q * 128, (q + 1) * 128)
            value = xs[rows, lanes]
            value_float = value.astype(F32)
            sides = (jnp.where(first, value_float, 0.0).astype(BF16), jnp.where(first, 0.0, value_float).astype(BF16))
            total = [jnp.where(first[0:half], skip[2 * q], skip[2 * q + 1]) * value_float[r * half:(r + 1) * half] for r in (0, 1)]
            for e in (0, 1):
                n = 2 * q + e
                ci = table[:, n:n + 1]
                cj = cjp[b, n:n + 1, :]
                for r in (0, 1):
                    lo, hi = r * half, (r + 1) * half
                    gap = jnp.minimum(ci[lo:hi] - cj[:, 0:hi], 0.0)
                    score = (jnp.exp2(gap) * cbm[lo:hi, 0:hi]).astype(BF16)
                    total[r] = total[r] + jnp.dot(score, sides[e][0:hi], preferred_element_type=F32)
            for r in (0, 1):
                local[pl.ds(pl.multiple_of(b * SPAN + r * half, half), half), lanes] = total[r]

    inside(0)

    pair.wait_recv()
    first_core = c == 0
    for n in range(4):
        own, far = whole_send[4 * c + n], pair_recv[n]
        own_through, far_through = from_parts(own[128:144]), from_parts(far[128:144])
        own_state, far_state = own[0:128].astype(F32), far[0:128].astype(F32)
        earlier = jnp.where(first_core, own_state, far_state)
        later = jnp.where(first_core, far_state, own_state)
        total = jnp.where(first_core, far_through, own_through) * earlier + later
        tail = in_parts(own_through * far_through)
        for r in range(4):
            chunk_send[n * 4 + r, 0:32, :] = total[r * 32:(r + 1) * 32].astype(BF16)
            chunk_send[n * 4 + r, 32:48, :] = tail

    @pl.loop(1, 16)
    def _(i):
        remote(chunk_send.at[(chip + i) % 16], chunk_recv.at[chip], chunk_ss, chunk_rs, same_core(i)).start()

    chunk_recv[chip] = chunk_send[chip]

    slice_send(2)
    inside(1)
    inside(2)
    for m in range(DIRECT_PIECES):
        for j in (0, 1):
            direct_copy(j, m).start()

    relay(0, 0)
    relay(0, 1)

    arrived = chunk_recv.at[pl.ds(0, 15)]
    chunk_all = remote(arrived, arrived, chunk_ss, chunk_rs, other)
    chunk_all.wait_recv()

    state = jnp.zeros((32, 128), F32)
    for t in range(16):
        inc_send[t] = state.astype(BF16)
        state = from_parts(chunk_recv[t, 32:48, :]) * state + chunk_recv[t, 0:32, :].astype(F32)

    @pl.loop(1, 16)
    def _(i):
        remote(inc_send.at[(chip + i) % 16], inc_recv.at[chip], inc_ss, inc_rs, same_core(i)).start()

    inc_recv[chip] = inc_send[chip]

    relay(1, 0)
    relay(1, 1)
    inside(3)
    relay(0, 2)

    returned = inc_recv.at[pl.ds(0, 15)]
    inc_all = remote(returned, returned, inc_ss, inc_rs, other)
    inc_all.wait_recv()
    for n in range(4):
        own, far = whole_send[4 * c + n], pair_recv[n]
        first_state = jnp.where(first_core, own[0:128].astype(F32), far[0:128].astype(F32))
        first_through = jnp.where(first_core, from_parts(own[128:144]), from_parts(far[128:144]))
        reaching = inc_recv[n * 4:(n + 1) * 4].reshape(STATE, 128)
        second = (first_through * reaching.astype(F32) + first_state).astype(BF16)
        incoming[4 * c + n] = jnp.where(first_core, reaching.astype(F32), second.astype(F32)).astype(BF16)
        pair_out[n] = jnp.where(first_core, second.astype(F32), reaching.astype(F32)).astype(BF16)
    handed = remote(pair_out, incoming.at[pl.ds(4 * c, 4)], last_ss, last_rs, other)
    handed.start()
    relay(2, 0)
    relay(2, 1)
    handed.wait_recv()
    copies_in[5].wait()
    copies_in[6].wait()

    def finish(b, put):
        rows = pl.ds(pl.multiple_of(b * SPAN, SPAN), SPAN)
        query = cmat[rows, :]

        def part(q, squares):
            lanes = pl.ds(pl.multiple_of(q * 128, 128), 128)
            state = (starts[b, q] + reach[b, q, 0:1, :] * incoming[q].astype(F32)).astype(BF16)
            inter = jnp.dot(query, state, preferred_element_type=F32)
            value = local[rows, lanes] + grow[rows, lanes] * inter
            v = gate[rows, lanes].astype(F32)
            gated = value * (v / (1.0 + jnp.exp(-v)))
            put(lanes, (gated * gain[:, lanes]).astype(BF16))
            return squares + gated * gated

        squares = lax.fori_loop(0, 8, part, jnp.zeros((SPAN, 128), F32))
        total = jnp.broadcast_to(jnp.sum(squares, axis=1, keepdims=True), (SPAN, 128)).T[0:16, :]
        high = total.astype(BF16).astype(F32)
        return jnp.where(iota((16, SPAN), 0) == 0, high, total - high).astype(BF16)

    def hid_copy(j):
        there = hid.at[h, pl.ds(pl.multiple_of(c * SPAN, SPAN), SPAN), :]
        return remote(hid_send.at[j], there, hid_ss.at[j], hid_rs.at[arrives_as[j]], (s, planes[j]))

    def far_copy(j):
        return remote(hid_send.at[j], hid_far.at[j], far_ss.at[j], far_rs.at[j], other)

    def product_copy(j):
        there = product_recv.at[arrives_as[j]]
        return remote(product_send.at[j], there, product_ss.at[j], product_rs.at[arrives_as[j]], (s, planes[j]))

    def product_all(j):
        part = product_recv.at[j]
        return remote(part, part, product_ss.at[j], product_rs.at[j], (s, planes[j]))


    there, here = (pl.ds(pl.multiple_of(core * SPAN, SPAN), SPAN) for core in (1 - c, c))

    def sum_copy(j):
        return remote(sums_send.at[j], sums.at[c, h], sum_ss, sum_rs, (s, planes[j]))

    for j in (2, 0, 1):
        def put(lanes, value, j=j):
            hid_send[j, :, lanes] = value

        sums_send[j] = finish(planes[j], put)
        hid_copy(j).start()
        sum_copy(j).start()
        if j < 2:
            far_copy(j).start()
        if j == 2:
            relay(1, 2)

    relay(3, 0)

    def put_own(lanes, value):
        hid[h, pl.ds(pl.multiple_of(c * SPAN, SPAN), SPAN), lanes] = value

    sums[c, h] = finish(h, put_own)

    def forward(n, plane):
        part = hid.at[plane, pl.ds(pl.multiple_of(c * SPAN, SPAN), SPAN), :]
        return remote(part, part, fwd_ss.at[n], fwd_rs.at[n], other)

    forward(3, h).start()

    own_weight.wait()
    for j in (0, 1):
        far_copy(j).wait_recv()
        for rows, value in ((here, hid_send), (there, hid_far)):
            product_send[j, rows, :] = jnp.dot(value[j], weight[h, :, PRODUCT], preferred_element_type=F32).astype(BF16)
        product_copy(j).start()

    relay(2, 2)
    relay(3, 1)

    forward(3, h).wait_recv()

    @pl.loop(0, 8)
    def _(n):
        lanes = pl.ds(pl.multiple_of(n * 256, 256), 256)
        acc[:, lanes] = jnp.dot(hid[h], weight[h, :, lanes], preferred_element_type=F32)

    def wait_hid(j):
        part = hid.at[planes[j], pl.ds(pl.multiple_of(c * SPAN, SPAN), SPAN), :]
        remote(part, part, hid_ss.at[j], hid_rs.at[j], (s, planes[j])).wait_recv()
        forward(j, planes[j]).start()

    def depth_of(k, last):
        first = (mine[k] // 8) * 512
        if last:
            first = 512 - first
        return pl.ds(pl.multiple_of(first, 512), 512)

    def multiply(j, last):
        for k in range(4):
            depth = depth_of(k, last)
            column, width = COLOURS[j][k]
            lanes = slice(column, column + width)
            acc[:, lanes] += jnp.dot(hid[planes[j], :, depth], weight[planes[j], depth, lanes], preferred_element_type=F32)

    wait_hid(2)
    forward(2, planes[2]).wait_recv()
    relay(3, 2)
    multiply(2, False)
    for j in (0, 1):
        wait_hid(j)
    totals = sums.at[c, pl.ds(0, 3)]
    remote(totals, totals, sum_ss, sum_rs, other).wait_recv()
    forward_sums = remote(sums.at[c], sums.at[c], fsum_ss, fsum_rs, other)
    forward_sums.start()
    for j in (0, 1):
        forward(j, planes[j]).wait_recv()
        multiply(j, False)

    forward_sums.wait_recv()

    def scales(core):
        total = jnp.zeros((16, SPAN), F32)
        for n in range(4):
            total = total + sums[core, n].astype(F32)
        both = lax.rsqrt((total[0:1] + total[1:2]) / INNER + 1e-05)
        return jnp.broadcast_to(both, (128, SPAN)).T

    scale_there, scale_here = scales(1 - c), scales(c)

    for j in (0, 1):
        step_all(3, j).wait_recv()
        multiply(j, True)
    for j in (0, 1):
        for m in range(DIRECT_PIECES):
            direct_wait(j, m)
        acc[:, DIRECT] += jnp.dot(hid[planes[j]], weight[planes[j], :, DIRECT], preferred_element_type=F32)
    for j in (0, 1):
        product_all(j).wait_recv()
    acc[:, PRODUCT] += product_recv[0].astype(F32) + product_recv[1].astype(F32)

    for n, (offset, width) in enumerate(LAST):
        step_all(3, 2, n).wait_recv()
        spans = [slice(k * 512 + offset, k * 512 + offset + width) for k in range(4)]
        columns = [pl.ds(pl.multiple_of(base + k * 512 + offset, 128), width) for k in range(4)]

        def ended(rows, scale):
            scale = jnp.concatenate([scale] * (width // 128), axis=1)
            terms = []
            for k in range(4):
                depth = depth_of(k, True)
                terms.append(jnp.dot(hid[planes[2], rows, depth], weight[planes[2], depth, spans[k]], preferred_element_type=F32))
            return [((acc[rows, spans[k]] + terms[k]) * scale).astype(BF16) for k in range(4)]

        for k, value in enumerate(ended(there, scale_there)):
            done[:, spans[k]] = value
        for k in range(4):
            remote(done.at[:, spans[k]], out.at[:, columns[k]], out_ss, out_rs, other).start()
        for k, value in enumerate(ended(here, scale_here)):
            out[:, columns[k]] = value

    for j in (0, 1, 2):
        slice_all(j).wait_send()
        for t in range(4):
            for n in range(step_parts(t, j)):
                step_all(t, j, n).wait_send()
        hid_copy(j).wait_send()
        forward(j, planes[j]).wait_send()
    totals_sent = remote(sums_send, sums_send, sum_ss, sum_rs, other)
    totals_sent.wait_send()
    for j in (0, 1):
        far_copy(j).wait_send()
        product_copy(j).wait_send()
        for m in range(DIRECT_PIECES):
            direct_copy(j, m).wait_send()
    forward(3, h).wait_send()
    forward_sums.wait_send()
    pair.wait_send()
    chunk_all.wait_send()
    inc_all.wait_send()
    handed.wait_send()
    whole = remote(done, done, out_ss, out_rs, other)
    whole.wait_send()
    whole.wait_recv()


def local(xs, gate_branch, bmat, cmat, dt_code, resets, decay_rate, skip, norm_gain, out_weight):
    vmem = pl.BlockSpec(memory_space=pltpu.VMEM)
    hbm = pl.BlockSpec(memory_space=pl.ANY)
    smem = pl.BlockSpec(memory_space=pltpu.SMEM)
    dma = pltpu.SemaphoreType.DMA
    V = pltpu.VMEM
    return pl.pallas_call(
        kernel,
        out_shape=pltpu.VMEM((256, 4096), BF16),
        in_specs=[hbm] * 8 + [smem, smem],
        out_specs=vmem,
        scratch_shapes=[
            V((1024, 1024), BF16),
            V((1024, 1024), BF16),
            V((1024, 128), BF16),
            V((1024, 128), BF16),
            V((16, 1024), jnp.int32),
            V((1, 1024), jnp.int32),
            V((1, 1024), F32),
            V((4, 1024, 2048), BF16),
            V((4, 512, 1024), BF16),
            V((3, 256, 1024), BF16),
            V((2, 256, 1024), BF16),
            V((2, 512, 512), BF16),
            V((2, 512, 512), BF16),
            V((2, 4, 16, 256), BF16),
            V((3, 16, 256), BF16),
            V((512, 2048), F32),
            V((256, 2048), BF16),
            V((256, 256), BF16),
            V((4, 256, 128), F32),
            V((4, 256, 256), BF16),
            V((4, 128, 256), BF16),
            V((4, 16, 256), F32),
            V((4, 8, 256), F32),
            V((1024, 1024), F32),
            V((4, 8, 128, 128), F32),
            V((4, 8, 8, 128), F32),
            V((8, 144, 128), BF16),
            V((4, 144, 128), BF16),
            V((16, 48, 128), BF16),
            V((16, 48, 128), BF16),
            V((16, 32, 128), BF16),
            V((16, 32, 128), BF16),
            V((4, 128, 128), BF16),
            V((8, 128, 128), BF16),
            V((256, 256), F32),
            V((1024, 1024), F32),
            dma((7,)), dma, dma((3,)), dma((3,)),
            dma((2, DIRECT_PIECES)), dma((2, DIRECT_PIECES)), dma((2,)), dma((2,)), dma((2,)), dma((2,)), dma((4, 5)), dma((4, 5)),
            dma, dma, dma, dma, dma, dma, dma, dma,
            dma((3,)), dma((3,)), dma, dma, dma((4,)), dma((4,)), dma, dma,
            dma, dma,
        ],
        compiler_params=pltpu.CompilerParams(
            collective_id=0, has_side_effects=True, vmem_limit_bytes=58 * 1024 * 1024
        ),
    )(
        xs, gate_branch, bmat, cmat, dt_code, resets.reshape(1, 1024), norm_gain.reshape(1, 1024), out_weight,
        decay_rate, skip,
    )


def solution(mesh):
    in_specs = (
        P("seq", "head"),
        P("seq", "head"),
        P("seq", None),
        P("seq", None),
        P("head", "seq"),
        P("seq"),
        P("head"),
        P("head"),
        P("head"),
        P("head", None),
    )
    out_specs = P(("seq", "head"), None)
    return jax.shard_map(local, mesh=mesh, in_specs=in_specs, out_specs=out_specs, check_vma=False)
```

```python
import jax
import jax.numpy as jnp
from jax import lax
from jax.experimental import pallas as pl
from jax.experimental.pallas import tpu as pltpu
from jax.sharding import PartitionSpec as P

HEAD_DIM = 64
STATE = 128
SPAN = 256
INNER = 4096
MESH = pl.DeviceIdType.MESH
LOG2E = 1.4426950408889634
F32 = jnp.float32
BF16 = jnp.bfloat16

COLOURS = (
    ((0, 384), (384, 256), (640, 384), (1024, 256)),
    ((0, 256), (256, 384), (640, 256), (896, 384)),
    ((0, 512), (512, 512), (1024, 512), (1536, 512)),
)
DIRECT = slice(1280, 1536)
DIRECT_PIECES = 2
PRODUCT = slice(1536, 2048)
LAST = ((0, 256), (256, 128), (384, 128))


def iota(shape, dim):
    return lax.broadcasted_iota(jnp.int32, shape, dim)


def kernel(
    xs_hbm, gate_hbm, bmat_hbm, cmat_hbm, dt_hbm, resets_hbm, gain_hbm, w_hbm, rate, skip,
    out,
    xs, gate, bmat, cmat, dt, resets, gain, weight, hid, hid_send, hid_far, product_send, product_recv, sums, sums_send, acc, done,
    tri, col, split, bt, cjp, cntrow, grow, starts, reach, whole_send, pair_recv, chunk_send, chunk_recv, inc_send, inc_recv,
    pair_out, incoming, cbm, local,
    in_sem, own_sem, slice_ss, slice_rs, direct_ss, direct_rs, far_ss, far_rs, product_ss, product_rs, step_ss, step_rs,
    pair_ss, pair_rs, chunk_ss, chunk_rs, inc_ss, inc_rs, last_ss, last_rs, hid_ss, hid_rs, sum_ss, sum_rs, fwd_ss, fwd_rs, fsum_ss, fsum_rs,
    out_ss, out_rs,
):
    s = lax.axis_index("seq")
    h = lax.axis_index("head")
    x, z, c = s // 8, (s // 2) % 4, s % 2
    other = (s + 1 - 2 * c, h)

    def remote(src, dst, ss, rs, dev):
        return pltpu.make_async_remote_copy(
            src_ref=src, dst_ref=dst, send_sem=ss, recv_sem=rs, device_id=dev, device_id_type=MESH
        )

    base = c * 2048
    own_weight = pltpu.make_async_copy(w_hbm.at[:, pl.ds(pl.multiple_of(base, 128), 2048)], weight.at[h], own_sem)
    own_weight.start()

    barrier = pltpu.get_barrier_semaphore()
    chip = s // 2

    def same_core(i):
        return ((chip + i) % 16 * 2 + c, h)

    @pl.loop(1, 16)
    def _(i):
        pl.semaphore_signal(barrier, inc=1, device_id=same_core(i), device_id_type=MESH)

    pl.semaphore_signal(barrier, inc=1, device_id=other, device_id_type=MESH)
    for d in (1, 2, 3):
        pl.semaphore_signal(barrier, inc=1, device_id=(s, (h + d) % 4), device_id_type=MESH)

    sources = (dt_hbm, resets_hbm, bmat_hbm, cmat_hbm, xs_hbm, gate_hbm, gain_hbm)
    places = (dt, resets, bmat, cmat, xs, gate, gain)
    copies_in = [pltpu.make_async_copy(a, b, in_sem.at[n]) for n, (a, b) in enumerate(zip(sources, places))]
    for cp in copies_in:
        cp.start()

    planes = [(h + 1) % 4, (h + 3) % 4, (h + 2) % 4]
    arrives_as = (1, 0, 2)

    px, pz = x % 2, z % 2
    ax, az = x // 2, z // 2
    bx, bz = ((x + 1) // 2) % 2, ((z + 1) // 2) % 2
    x_a, z_a = x + 1 - 2 * px, z + 1 - 2 * pz
    x_b, z_b = (x + 3 + 2 * px) % 4, (z + 3 + 2 * pz) % 4

    def at(xx, zz):
        return ((xx * 4 + zz) * 2 + c, h)

    along = (at(x_a, z), at(x, z_a), at(x_b, z), at(x, z_b))
    bits = ((px, pz, ax, az), (pz, px, az, bx), (px, pz, bx, bz), (pz, px, bz, ax))
    mine = [b0 + 2 * b1 + 4 * b2 + 8 * b3 for b0, b1, b2, b3 in bits]

    def slice_send(j):
        for k in range(4):
            first, width = COLOURS[arrives_as[j]][k]
            rows = pl.ds(pl.multiple_of(mine[k] * 64, 64), 64)
            part = weight.at[h, rows, pl.ds(first, width)]
            remote(part, part, slice_ss.at[j], slice_rs.at[arrives_as[j]], (s, planes[j])).start()

    def amount(t, j):
        return weight.at[planes[j], pl.ds(0, 64 << t), pl.ds(0, 2048 if j == 2 else 1280)]

    def slice_all(j):
        part = amount(0, j)
        return remote(part, part, slice_ss.at[arrives_as[j]], slice_rs.at[j], (s, planes[j]))

    per = 1024 // DIRECT_PIECES

    def direct_copy(j, m):
        rows = pl.ds(m * per, per)
        part = weight.at[h, rows, pl.ds(1280, 256)]
        return remote(part, part, direct_ss.at[j, m], direct_rs.at[1 - j, m], (s, planes[j]))

    def direct_wait(j, m):
        part = weight.at[planes[j], pl.ds(m * per, per), pl.ds(1280, 256)]
        remote(part, part, direct_ss.at[j, m], direct_rs.at[j, m], (s, planes[j])).wait_recv()

    def step_parts(t, j):
        return len(LAST) if (t, j) == (3, 2) else 1

    def step_all(t, j, n=0):
        part = amount(t, j)
        if (t, j) == (3, 2):
            part = weight.at[planes[j], pl.ds(0, 512), pl.ds(0, 4 * LAST[n][1])]
        return remote(part, part, step_ss.at[t, j + n], step_rs.at[t, j + n], other)

    def step_send(t, j):
        for n in range(step_parts(t, j)):
            for k in range(4):
                column, width = COLOURS[j][k]
                if (t, j) == (3, 2):
                    column, width = column + LAST[n][0], LAST[n][1]
                first = (mine[k] // (1 << t)) * (64 << t)
                rows = pl.ds(pl.multiple_of(first, 64 << t), 64 << t)
                part = weight.at[planes[j], rows, pl.ds(column, width)]
                remote(part, part, step_ss.at[t, j + n], step_rs.at[t, j + n], along[(k + t) % 4]).start()

    def relay(t, j):
        if t == 0:
            slice_all(j).wait_recv()
        else:
            step_all(t - 1, j).wait_recv()
        step_send(t, j)

    pl.semaphore_wait(barrier, 19)
    own_weight.wait()

    slice_send(0)
    slice_send(1)

    tri[...] = jnp.where(iota((SPAN, SPAN), 0) <= iota((SPAN, SPAN), 1), 1.0, 0.0).astype(BF16)
    for n in (0, 1, 2):
        copies_in[n].wait()
    head_row = iota((16, SPAN), 0)
    slope = jnp.zeros((16, SPAN), F32)
    for n in range(16):
        slope = jnp.where(head_row == n, rate[n] * (-LOG2E / 16.0), slope)
    for b in range(4):
        d = dt[:, b * SPAN:(b + 1) * SPAN]
        flags = jnp.broadcast_to(resets[:, b * SPAN:(b + 1) * SPAN], (16, SPAN))
        parts = [d & 0xFF, d & 0xFF00, d & 0x30000, flags]
        stack = jnp.concatenate([p.astype(F32) for p in parts], axis=0).astype(BF16)
        run = jnp.dot(stack, tri[...], preferred_element_type=F32)
        c2 = (run[0:16] + run[16:32] + run[32:48]) * slope
        count = run[48:64]
        ls = jnp.log(jnp.minimum(d.astype(F32) * 0.0625, 1.0)) * LOG2E
        c2_end, count_end = c2[:, SPAN - 1:SPAN], count[:, SPAN - 1:SPAN]
        from_start = jnp.where(count == 0, jnp.exp2(c2), 0.0)
        to_end = jnp.where(count == count_end, jnp.exp2(c2_end - c2 + ls), 0.0)
        cjp[b] = c2 - ls
        cntrow[b] = count[0:8]
        table = jnp.concatenate([c2, from_start, to_end, count, jnp.zeros((64, SPAN), F32)], axis=0)
        flipped = table.T
        col[b] = flipped
        high = flipped.astype(BF16)
        low = (flipped - high.astype(F32)).astype(BF16)
        split[b] = jnp.concatenate([high, low], axis=1)
        bt[b] = bmat[b * SPAN:(b + 1) * SPAN, :].T

    copies_in[3].wait()
    copies_in[4].wait()

    def in_parts(row):
        high = row.astype(BF16).astype(F32)
        mid = (row - high).astype(BF16).astype(F32)
        line = iota((16, 128), 0)
        low = row - high - mid
        return jnp.where(line == 0, high, jnp.where(line == 1, mid, jnp.where(line == 2, low, 0.0))).astype(BF16)

    def from_parts(rows):
        rows = rows.astype(F32)
        return rows[0:1] + rows[1:2] + rows[2:3]

    def states(group):
        row, lane = iota((SPAN, SPAN), 0) % 128, iota((SPAN, SPAN), 1)
        wides, fresh = {}, {}
        for q in group:
            pick = jnp.where(lane < 128, 16, 32) + 2 * q + (lane % 128) // 64
            pick = jnp.where(row == pick, 1.0, 0.0).astype(BF16)
            for b in range(4):
                wides[q, b] = jnp.dot(split[b], pick, preferred_element_type=F32)
        for q in group:
            lanes = slice(q * 128, (q + 1) * 128)
            for b in range(4):
                rows = slice(b * SPAN, (b + 1) * SPAN)
                grow[rows, lanes] = wides[q, b][:, 0:128]
                weighted = (xs[rows, lanes].astype(F32) * wides[q, b][:, 128:256]).astype(BF16)
                fresh[q, b] = jnp.dot(bt[b], weighted, preferred_element_type=F32)
        for q in group:
            run = jnp.zeros((STATE, 128), F32)
            product = jnp.ones((1, 128), F32)
            for b in range(4):
                starts[b, q] = run
                reach[b, q] = jnp.broadcast_to(product, (8, 128))
                through = wides[q, b][SPAN - 1:SPAN, 0:128]
                run = through * run + fresh[q, b]
                product = product * through
            whole_send[q, 0:128, :] = run.astype(BF16)
            whole_send[q, 128:144, :] = in_parts(product)

    for q in range(0, 8, 2):
        states((q, q + 1))

    theirs = whole_send.at[pl.ds(4 - 4 * c, 4)]
    pair = remote(theirs, pair_recv, pair_ss, pair_rs, other)
    pair.start()

    half = SPAN // 2

    def inside(b):
        rows = pl.ds(pl.multiple_of(b * SPAN, SPAN), SPAN)
        table = col[b]
        pair = jnp.dot(cmat[rows, :], bt[b], preferred_element_type=F32)
        same = (table[:, 48:49] == cntrow[b][0:1, :]) & (iota((SPAN, SPAN), 1) <= iota((SPAN, SPAN), 0))
        cbm[...] = jnp.where(same, pair, 0.0)
        first = iota((SPAN, 128), 1) < HEAD_DIM
        for q in range(8):
            lanes = slice(q * 128, (q + 1) * 128)
            value = xs[rows, lanes]
            value_float = value.astype(F32)
            sides = (jnp.where(first, value_float, 0.0).astype(BF16), jnp.where(first, 0.0, value_float).astype(BF16))
            total = [jnp.where(first[0:half], skip[2 * q], skip[2 * q + 1]) * value_float[r * half:(r + 1) * half] for r in (0, 1)]
            for e in (0, 1):
                n = 2 * q + e
                ci = table[:, n:n + 1]
                cj = cjp[b, n:n + 1, :]
                for r in (0, 1):
                    lo, hi = r * half, (r + 1) * half
                    gap = jnp.minimum(ci[lo:hi] - cj[:, 0:hi], 0.0)
                    score = (jnp.exp2(gap) * cbm[lo:hi, 0:hi]).astype(BF16)
                    total[r] = total[r] + jnp.dot(score, sides[e][0:hi], preferred_element_type=F32)
            for r in (0, 1):
                local[pl.ds(pl.multiple_of(b * SPAN + r * half, half), half), lanes] = total[r]

    inside(0)

    pair.wait_recv()
    first_core = c == 0
    for n in range(4):
        own, far = whole_send[4 * c + n], pair_recv[n]
        own_through, far_through = from_parts(own[128:144]), from_parts(far[128:144])
        own_state, far_state = own[0:128].astype(F32), far[0:128].astype(F32)
        earlier = jnp.where(first_core, own_state, far_state)
        later = jnp.where(first_core, far_state, own_state)
        total = jnp.where(first_core, far_through, own_through) * earlier + later
        tail = in_parts(own_through * far_through)
        for r in range(4):
            chunk_send[n * 4 + r, 0:32, :] = total[r * 32:(r + 1) * 32].astype(BF16)
            chunk_send[n * 4 + r, 32:48, :] = tail

    @pl.loop(1, 16)
    def _(i):
        remote(chunk_send.at[(chip + i) % 16], chunk_recv.at[chip], chunk_ss, chunk_rs, same_core(i)).start()

    chunk_recv[chip] = chunk_send[chip]

    slice_send(2)
    inside(1)
    inside(2)
    for m in range(DIRECT_PIECES):
        for j in (0, 1):
            direct_copy(j, m).start()

    relay(0, 0)
    relay(0, 1)

    arrived = chunk_recv.at[pl.ds(0, 15)]
    chunk_all = remote(arrived, arrived, chunk_ss, chunk_rs, other)
    chunk_all.wait_recv()

    state = jnp.zeros((32, 128), F32)
    for t in range(16):
        inc_send[t] = state.astype(BF16)
        state = from_parts(chunk_recv[t, 32:48, :]) * state + chunk_recv[t, 0:32, :].astype(F32)

    @pl.loop(1, 16)
    def _(i):
        remote(inc_send.at[(chip + i) % 16], inc_recv.at[chip], inc_ss, inc_rs, same_core(i)).start()

    inc_recv[chip] = inc_send[chip]

    relay(1, 0)
    relay(1, 1)
    inside(3)
    relay(0, 2)

    returned = inc_recv.at[pl.ds(0, 15)]
    inc_all = remote(returned, returned, inc_ss, inc_rs, other)
    inc_all.wait_recv()
    for n in range(4):
        own, far = whole_send[4 * c + n], pair_recv[n]
        first_state = jnp.where(first_core, own[0:128].astype(F32), far[0:128].astype(F32))
        first_through = jnp.where(first_core, from_parts(own[128:144]), from_parts(far[128:144]))
        reaching = inc_recv[n * 4:(n + 1) * 4].reshape(STATE, 128)
        second = (first_through * reaching.astype(F32) + first_state).astype(BF16)
        incoming[4 * c + n] = jnp.where(first_core, reaching.astype(F32), second.astype(F32)).astype(BF16)
        pair_out[n] = jnp.where(first_core, second.astype(F32), reaching.astype(F32)).astype(BF16)
    handed = remote(pair_out, incoming.at[pl.ds(4 * c, 4)], last_ss, last_rs, other)
    handed.start()
    relay(2, 0)
    relay(2, 1)
    handed.wait_recv()
    copies_in[5].wait()
    copies_in[6].wait()

    def finish(b, put):
        rows = pl.ds(pl.multiple_of(b * SPAN, SPAN), SPAN)
        query = cmat[rows, :]

        def part(q, squares):
            lanes = pl.ds(pl.multiple_of(q * 128, 128), 128)
            state = (starts[b, q] + reach[b, q, 0:1, :] * incoming[q].astype(F32)).astype(BF16)
            inter = jnp.dot(query, state, preferred_element_type=F32)
            value = local[rows, lanes] + grow[rows, lanes] * inter
            v = gate[rows, lanes].astype(F32)
            gated = value * (v / (1.0 + jnp.exp(-v)))
            put(lanes, (gated * gain[:, lanes]).astype(BF16))
            return squares + gated * gated

        squares = lax.fori_loop(0, 8, part, jnp.zeros((SPAN, 128), F32))
        total = jnp.broadcast_to(jnp.sum(squares, axis=1, keepdims=True), (SPAN, 128)).T[0:16, :]
        high = total.astype(BF16).astype(F32)
        return jnp.where(iota((16, SPAN), 0) == 0, high, total - high).astype(BF16)

    def hid_copy(j):
        there = hid.at[h, pl.ds(pl.multiple_of(c * SPAN, SPAN), SPAN), :]
        return remote(hid_send.at[j], there, hid_ss.at[j], hid_rs.at[arrives_as[j]], (s, planes[j]))

    def far_copy(j):
        return remote(hid_send.at[j], hid_far.at[j], far_ss.at[j], far_rs.at[j], other)

    def product_copy(j):
        there = product_recv.at[arrives_as[j]]
        return remote(product_send.at[j], there, product_ss.at[j], product_rs.at[arrives_as[j]], (s, planes[j]))

    def product_all(j):
        part = product_recv.at[j]
        return remote(part, part, product_ss.at[j], product_rs.at[j], (s, planes[j]))


    there, here = (pl.ds(pl.multiple_of(core * SPAN, SPAN), SPAN) for core in (1 - c, c))

    def sum_copy(j):
        return remote(sums_send.at[j], sums.at[c, h], sum_ss, sum_rs, (s, planes[j]))

    for j in (2, 0, 1):
        def put(lanes, value, j=j):
            hid_send[j, :, lanes] = value

        sums_send[j] = finish(planes[j], put)
        hid_copy(j).start()
        sum_copy(j).start()
        if j < 2:
            far_copy(j).start()
        if j == 2:
            relay(1, 2)

    relay(3, 0)

    def put_own(lanes, value):
        hid[h, pl.ds(pl.multiple_of(c * SPAN, SPAN), SPAN), lanes] = value

    sums[c, h] = finish(h, put_own)

    def forward(n, plane):
        part = hid.at[plane, pl.ds(pl.multiple_of(c * SPAN, SPAN), SPAN), :]
        return remote(part, part, fwd_ss.at[n], fwd_rs.at[n], other)

    forward(3, h).start()

    for j in (0, 1):
        far_copy(j).wait_recv()
        for rows, value in ((here, hid_send), (there, hid_far)):
            product_send[j, rows, :] = jnp.dot(value[j], weight[h, :, PRODUCT], preferred_element_type=F32).astype(BF16)
        product_copy(j).start()

    relay(2, 2)
    relay(3, 1)

    forward(3, h).wait_recv()

    @pl.loop(0, 8)
    def _(n):
        lanes = pl.ds(pl.multiple_of(n * 256, 256), 256)
        acc[:, lanes] = jnp.dot(hid[h], weight[h, :, lanes], preferred_element_type=F32)

    def wait_hid(j):
        part = hid.at[planes[j], pl.ds(pl.multiple_of(c * SPAN, SPAN), SPAN), :]
        remote(part, part, hid_ss.at[j], hid_rs.at[j], (s, planes[j])).wait_recv()
        forward(j, planes[j]).start()

    def depth_of(k, last):
        first = (mine[k] // 8) * 512
        if last:
            first = 512 - first
        return pl.ds(pl.multiple_of(first, 512), 512)

    def multiply(j, last):
        for k in range(4):
            depth = depth_of(k, last)
            column, width = COLOURS[j][k]
            lanes = slice(column, column + width)
            acc[:, lanes] += jnp.dot(hid[planes[j], :, depth], weight[planes[j], depth, lanes], preferred_element_type=F32)

    wait_hid(2)
    forward(2, planes[2]).wait_recv()
    relay(3, 2)
    multiply(2, False)
    for j in (0, 1):
        wait_hid(j)
    totals = sums.at[c, pl.ds(0, 3)]
    remote(totals, totals, sum_ss, sum_rs, other).wait_recv()
    forward_sums = remote(sums.at[c], sums.at[c], fsum_ss, fsum_rs, other)
    forward_sums.start()
    for j in (0, 1):
        forward(j, planes[j]).wait_recv()
        multiply(j, False)

    forward_sums.wait_recv()

    def scales(core):
        total = jnp.zeros((16, SPAN), F32)
        for n in range(4):
            total = total + sums[core, n].astype(F32)
        both = lax.rsqrt((total[0:1] + total[1:2]) / INNER + 1e-05)
        return jnp.broadcast_to(both, (128, SPAN)).T

    scale_there, scale_here = scales(1 - c), scales(c)

    for j in (0, 1):
        step_all(3, j).wait_recv()
        multiply(j, True)
    for j in (0, 1):
        for m in range(DIRECT_PIECES):
            direct_wait(j, m)
        acc[:, DIRECT] += jnp.dot(hid[planes[j]], weight[planes[j], :, DIRECT], preferred_element_type=F32)
    def finish_part(n, colours):
        offset, width = LAST[n]
        spans = {k: slice(k * 512 + offset, k * 512 + offset + width) for k in colours}
        columns = {k: pl.ds(pl.multiple_of(base + k * 512 + offset, 128), width) for k in colours}

        def ended(rows, scale):
            scale = jnp.concatenate([scale] * (width // 128), axis=1)
            terms = {}
            for k in colours:
                depth = depth_of(k, True)
                terms[k] = jnp.dot(hid[planes[2], rows, depth], weight[planes[2], depth, spans[k]], preferred_element_type=F32)
            return {k: ((acc[rows, spans[k]] + terms[k]) * scale).astype(BF16) for k in colours}

        for k, value in ended(there, scale_there).items():
            done[:, spans[k]] = value
        for k in colours:
            remote(done.at[:, spans[k]], out.at[:, columns[k]], out_ss, out_rs, other).start()
        for k, value in ended(here, scale_here).items():
            out[:, columns[k]] = value

    early, late = (0, 1, 2), (3,)
    for n in (0, 1):
        step_all(3, 2, n).wait_recv()
        finish_part(n, early)
    for j in (0, 1):
        product_all(j).wait_recv()
    acc[:, PRODUCT] += product_recv[0].astype(F32) + product_recv[1].astype(F32)
    for n in (0, 1):
        finish_part(n, late)
    step_all(3, 2, 2).wait_recv()
    finish_part(2, early + late)

    for j in (0, 1, 2):
        slice_all(j).wait_send()
        for t in range(4):
            for n in range(step_parts(t, j)):
                step_all(t, j, n).wait_send()
        hid_copy(j).wait_send()
        forward(j, planes[j]).wait_send()
    totals_sent = remote(sums_send, sums_send, sum_ss, sum_rs, other)
    totals_sent.wait_send()
    for j in (0, 1):
        far_copy(j).wait_send()
        product_copy(j).wait_send()
        for m in range(DIRECT_PIECES):
            direct_copy(j, m).wait_send()
    forward(3, h).wait_send()
    forward_sums.wait_send()
    pair.wait_send()
    chunk_all.wait_send()
    inc_all.wait_send()
    handed.wait_send()
    whole = remote(done, done, out_ss, out_rs, other)
    whole.wait_send()
    whole.wait_recv()


def local(xs, gate_branch, bmat, cmat, dt_code, resets, decay_rate, skip, norm_gain, out_weight):
    vmem = pl.BlockSpec(memory_space=pltpu.VMEM)
    hbm = pl.BlockSpec(memory_space=pl.ANY)
    smem = pl.BlockSpec(memory_space=pltpu.SMEM)
    dma = pltpu.SemaphoreType.DMA
    V = pltpu.VMEM
    return pl.pallas_call(
        kernel,
        out_shape=pltpu.VMEM((256, 4096), BF16),
        in_specs=[hbm] * 8 + [smem, smem],
        out_specs=vmem,
        scratch_shapes=[
            V((1024, 1024), BF16),
            V((1024, 1024), BF16),
            V((1024, 128), BF16),
            V((1024, 128), BF16),
            V((16, 1024), jnp.int32),
            V((1, 1024), jnp.int32),
            V((1, 1024), F32),
            V((4, 1024, 2048), BF16),
            V((4, 512, 1024), BF16),
            V((3, 256, 1024), BF16),
            V((2, 256, 1024), BF16),
            V((2, 512, 512), BF16),
            V((2, 512, 512), BF16),
            V((2, 4, 16, 256), BF16),
            V((3, 16, 256), BF16),
            V((512, 2048), F32),
            V((256, 2048), BF16),
            V((256, 256), BF16),
            V((4, 256, 128), F32),
            V((4, 256, 256), BF16),
            V((4, 128, 256), BF16),
            V((4, 16, 256), F32),
            V((4, 8, 256), F32),
            V((1024, 1024), F32),
            V((4, 8, 128, 128), F32),
            V((4, 8, 8, 128), F32),
            V((8, 144, 128), BF16),
            V((4, 144, 128), BF16),
            V((16, 48, 128), BF16),
            V((16, 48, 128), BF16),
            V((16, 32, 128), BF16),
            V((16, 32, 128), BF16),
            V((4, 128, 128), BF16),
            V((8, 128, 128), BF16),
            V((256, 256), F32),
            V((1024, 1024), F32),
            dma((7,)), dma, dma((3,)), dma((3,)),
            dma((2, DIRECT_PIECES)), dma((2, DIRECT_PIECES)), dma((2,)), dma((2,)), dma((2,)), dma((2,)), dma((4, 5)), dma((4, 5)),
            dma, dma, dma, dma, dma, dma, dma, dma,
            dma((3,)), dma((3,)), dma, dma, dma((4,)), dma((4,)), dma, dma,
            dma, dma,
        ],
        compiler_params=pltpu.CompilerParams(
            collective_id=0, has_side_effects=True, vmem_limit_bytes=58 * 1024 * 1024
        ),
    )(
        xs, gate_branch, bmat, cmat, dt_code, resets.reshape(1, 1024), norm_gain.reshape(1, 1024), out_weight,
        decay_rate, skip,
    )


def solution(mesh):
    in_specs = (
        P("seq", "head"),
        P("seq", "head"),
        P("seq", None),
        P("seq", None),
        P("head", "seq"),
        P("seq"),
        P("head"),
        P("head"),
        P("head"),
        P("head", None),
    )
    out_specs = P(("seq", "head"), None)
    return jax.shard_map(local, mesh=mesh, in_specs=in_specs, out_specs=out_specs, check_vma=False)
```

```python
import jax
import jax.numpy as jnp
from jax import lax
from jax.experimental import pallas as pl
from jax.experimental.pallas import tpu as pltpu
from jax.sharding import PartitionSpec as P

HEAD_DIM = 64
STATE = 128
SPAN = 256
INNER = 4096
MESH = pl.DeviceIdType.MESH
LOG2E = 1.4426950408889634
F32 = jnp.float32
BF16 = jnp.bfloat16

COLOURS = (
    ((0, 384), (384, 256), (640, 384), (1024, 256)),
    ((0, 256), (256, 384), (640, 256), (896, 384)),
    ((0, 512), (512, 512), (1024, 512), (1536, 512)),
)
DIRECT = slice(1280, 1536)
DIRECT_PIECES = 2
PRODUCT = slice(1536, 2048)
LAST = ((0, 256), (256, 128), (384, 128))


def iota(shape, dim):
    return lax.broadcasted_iota(jnp.int32, shape, dim)


def kernel(
    xs_hbm, gate_hbm, bmat_hbm, cmat_hbm, dt_hbm, resets_hbm, gain_hbm, w_hbm, rate_hbm, skip_hbm,
    out,
    rate, skip, xs, gate, bmat, cmat, dt, resets, gain, weight, hid, hid_send, hid_far, product_send, product_recv, sums, sums_send, acc, done,
    tri, col, split, bt, cjp, cntrow, grow, starts, reach, whole_send, pair_recv, chunk_send, chunk_recv, inc_send, inc_recv,
    pair_out, incoming, cbm, local,
    in_sem, own_sem, slice_ss, slice_rs, direct_ss, direct_rs, far_ss, far_rs, product_ss, product_rs, step_ss, step_rs,
    pair_ss, pair_rs, chunk_ss, chunk_rs, inc_ss, inc_rs, last_ss, last_rs, hid_ss, hid_rs, sum_ss, sum_rs, fwd_ss, fwd_rs, fsum_ss, fsum_rs,
    out_ss, out_rs,
):
    s = lax.axis_index("seq")
    h = lax.axis_index("head")
    x, z, c = s // 8, (s // 2) % 4, s % 2
    other = (s + 1 - 2 * c, h)

    def remote(src, dst, ss, rs, dev):
        return pltpu.make_async_remote_copy(
            src_ref=src, dst_ref=dst, send_sem=ss, recv_sem=rs, device_id=dev, device_id_type=MESH
        )

    base = c * 2048
    own_weight = pltpu.make_async_copy(w_hbm.at[:, pl.ds(pl.multiple_of(base, 128), 2048)], weight.at[h], own_sem)
    own_weight.start()

    barrier = pltpu.get_barrier_semaphore()
    chip = s // 2

    def same_core(i):
        return ((chip + i) % 16 * 2 + c, h)

    @pl.loop(1, 16)
    def _(i):
        pl.semaphore_signal(barrier, inc=1, device_id=same_core(i), device_id_type=MESH)

    pl.semaphore_signal(barrier, inc=1, device_id=other, device_id_type=MESH)
    for d in (1, 2, 3):
        pl.semaphore_signal(barrier, inc=1, device_id=(s, (h + d) % 4), device_id_type=MESH)

    sources = (dt_hbm, resets_hbm, bmat_hbm, cmat_hbm, xs_hbm, gate_hbm, gain_hbm, rate_hbm, skip_hbm)
    places = (dt, resets, bmat, cmat, xs, gate, gain, rate, skip)
    copies_in = [pltpu.make_async_copy(a, b, in_sem.at[n]) for n, (a, b) in enumerate(zip(sources, places))]
    for cp in copies_in:
        cp.start()

    planes = [(h + 1) % 4, (h + 3) % 4, (h + 2) % 4]
    arrives_as = (1, 0, 2)

    px, pz = x % 2, z % 2
    ax, az = x // 2, z // 2
    bx, bz = ((x + 1) // 2) % 2, ((z + 1) // 2) % 2
    x_a, z_a = x + 1 - 2 * px, z + 1 - 2 * pz
    x_b, z_b = (x + 3 + 2 * px) % 4, (z + 3 + 2 * pz) % 4

    def at(xx, zz):
        return ((xx * 4 + zz) * 2 + c, h)

    along = (at(x_a, z), at(x, z_a), at(x_b, z), at(x, z_b))
    bits = ((px, pz, ax, az), (pz, px, az, bx), (px, pz, bx, bz), (pz, px, bz, ax))
    mine = [b0 + 2 * b1 + 4 * b2 + 8 * b3 for b0, b1, b2, b3 in bits]

    def slice_send(j):
        for k in range(4):
            first, width = COLOURS[arrives_as[j]][k]
            rows = pl.ds(pl.multiple_of(mine[k] * 64, 64), 64)
            part = weight.at[h, rows, pl.ds(first, width)]
            remote(part, part, slice_ss.at[j], slice_rs.at[arrives_as[j]], (s, planes[j])).start()

    def amount(t, j):
        return weight.at[planes[j], pl.ds(0, 64 << t), pl.ds(0, 2048 if j == 2 else 1280)]

    def slice_all(j):
        part = amount(0, j)
        return remote(part, part, slice_ss.at[arrives_as[j]], slice_rs.at[j], (s, planes[j]))

    per = 1024 // DIRECT_PIECES

    def direct_copy(j, m):
        rows = pl.ds(m * per, per)
        part = weight.at[h, rows, pl.ds(1280, 256)]
        return remote(part, part, direct_ss.at[j, m], direct_rs.at[1 - j, m], (s, planes[j]))

    def direct_wait(j, m):
        part = weight.at[planes[j], pl.ds(m * per, per), pl.ds(1280, 256)]
        remote(part, part, direct_ss.at[j, m], direct_rs.at[j, m], (s, planes[j])).wait_recv()

    def step_parts(t, j):
        return len(LAST) if (t, j) == (3, 2) else 1

    def step_all(t, j, n=0):
        part = amount(t, j)
        if (t, j) == (3, 2):
            part = weight.at[planes[j], pl.ds(0, 512), pl.ds(0, 4 * LAST[n][1])]
        return remote(part, part, step_ss.at[t, j + n], step_rs.at[t, j + n], other)

    def step_send(t, j):
        for n in range(step_parts(t, j)):
            for k in range(4):
                column, width = COLOURS[j][k]
                if (t, j) == (3, 2):
                    column, width = column + LAST[n][0], LAST[n][1]
                first = (mine[k] // (1 << t)) * (64 << t)
                rows = pl.ds(pl.multiple_of(first, 64 << t), 64 << t)
                part = weight.at[planes[j], rows, pl.ds(column, width)]
                remote(part, part, step_ss.at[t, j + n], step_rs.at[t, j + n], along[(k + t) % 4]).start()

    def relay(t, j):
        if t == 0:
            slice_all(j).wait_recv()
        else:
            step_all(t - 1, j).wait_recv()
        step_send(t, j)

    pl.semaphore_wait(barrier, 19)
    own_weight.wait()

    slice_send(0)
    slice_send(1)

    tri[...] = jnp.where(iota((SPAN, SPAN), 0) <= iota((SPAN, SPAN), 1), 1.0, 0.0).astype(BF16)
    for n in (0, 1, 2, 7, 8):
        copies_in[n].wait()
    head_row = iota((16, SPAN), 0)
    slope = jnp.zeros((16, SPAN), F32)
    for n in range(16):
        slope = jnp.where(head_row == n, rate[n] * (-LOG2E / 16.0), slope)
    for b in range(4):
        d = dt[:, b * SPAN:(b + 1) * SPAN]
        flags = jnp.broadcast_to(resets[:, b * SPAN:(b + 1) * SPAN], (16, SPAN))
        parts = [d & 0xFF, d & 0xFF00, d & 0x30000, flags]
        stack = jnp.concatenate([p.astype(F32) for p in parts], axis=0).astype(BF16)
        run = jnp.dot(stack, tri[...], preferred_element_type=F32)
        c2 = (run[0:16] + run[16:32] + run[32:48]) * slope
        count = run[48:64]
        ls = jnp.log(jnp.minimum(d.astype(F32) * 0.0625, 1.0)) * LOG2E
        c2_end, count_end = c2[:, SPAN - 1:SPAN], count[:, SPAN - 1:SPAN]
        from_start = jnp.where(count == 0, jnp.exp2(c2), 0.0)
        to_end = jnp.where(count == count_end, jnp.exp2(c2_end - c2 + ls), 0.0)
        cjp[b] = c2 - ls
        cntrow[b] = count[0:8]
        table = jnp.concatenate([c2, from_start, to_end, count, jnp.zeros((64, SPAN), F32)], axis=0)
        flipped = table.T
        col[b] = flipped
        high = flipped.astype(BF16)
        low = (flipped - high.astype(F32)).astype(BF16)
        split[b] = jnp.concatenate([high, low], axis=1)
        bt[b] = bmat[b * SPAN:(b + 1) * SPAN, :].T

    copies_in[3].wait()
    copies_in[4].wait()

    def in_parts(row):
        high = row.astype(BF16).astype(F32)
        mid = (row - high).astype(BF16).astype(F32)
        line = iota((8, 128), 0)
        low = row - high - mid
        return jnp.where(line == 0, high, jnp.where(line == 1, mid, jnp.where(line == 2, low, 0.0))).astype(BF16)

    def from_parts(rows):
        rows = rows.astype(F32)
        return rows[0:1] + rows[1:2] + rows[2:3]

    def states(group):
        row, lane = iota((SPAN, SPAN), 0) % 128, iota((SPAN, SPAN), 1)
        wides, fresh = {}, {}
        for q in group:
            pick = jnp.where(lane < 128, 16, 32) + 2 * q + (lane % 128) // 64
            pick = jnp.where(row == pick, 1.0, 0.0).astype(BF16)
            for b in range(4):
                wides[q, b] = jnp.dot(split[b], pick, preferred_element_type=F32)
        for q in group:
            lanes = slice(q * 128, (q + 1) * 128)
            for b in range(4):
                rows = slice(b * SPAN, (b + 1) * SPAN)
                grow[rows, lanes] = wides[q, b][:, 0:128]
                weighted = (xs[rows, lanes].astype(F32) * wides[q, b][:, 128:256]).astype(BF16)
                fresh[q, b] = jnp.dot(bt[b], weighted, preferred_element_type=F32)
        for q in group:
            run = jnp.zeros((STATE, 128), F32)
            product = jnp.ones((1, 128), F32)
            for b in range(4):
                starts[b, q] = run
                reach[b, q] = jnp.broadcast_to(product, (8, 128))
                through = wides[q, b][SPAN - 1:SPAN, 0:128]
                run = through * run + fresh[q, b]
                product = product * through
            whole_send[q, 0:128, :] = run.astype(BF16)
            whole_send[q, 128:136, :] = in_parts(product)

    for q in range(0, 8, 2):
        states((q, q + 1))

    theirs = whole_send.at[pl.ds(4 - 4 * c, 4)]
    pair = remote(theirs, pair_recv, pair_ss, pair_rs, other)
    pair.start()

    half = SPAN // 2

    def inside(b):
        rows = pl.ds(pl.multiple_of(b * SPAN, SPAN), SPAN)
        table = col[b]
        pair = jnp.dot(cmat[rows, :], bt[b], preferred_element_type=F32)
        same = (table[:, 48:49] == cntrow[b][0:1, :]) & (iota((SPAN, SPAN), 1) <= iota((SPAN, SPAN), 0))
        cbm[...] = jnp.where(same, pair, 0.0)
        first = iota((SPAN, 128), 1) < HEAD_DIM
        for q in range(8):
            lanes = slice(q * 128, (q + 1) * 128)
            value = xs[rows, lanes]
            value_float = value.astype(F32)
            sides = (jnp.where(first, value_float, 0.0).astype(BF16), jnp.where(first, 0.0, value_float).astype(BF16))
            total = [jnp.where(first[0:half], skip[2 * q], skip[2 * q + 1]) * value_float[r * half:(r + 1) * half] for r in (0, 1)]
            for e in (0, 1):
                n = 2 * q + e
                ci = table[:, n:n + 1]
                cj = cjp[b, n:n + 1, :]
                for r in (0, 1):
                    lo, hi = r * half, (r + 1) * half
                    gap = jnp.minimum(ci[lo:hi] - cj[:, 0:hi], 0.0)
                    score = (jnp.exp2(gap) * cbm[lo:hi, 0:hi]).astype(BF16)
                    total[r] = total[r] + jnp.dot(score, sides[e][0:hi], preferred_element_type=F32)
            for r in (0, 1):
                local[pl.ds(pl.multiple_of(b * SPAN + r * half, half), half), lanes] = total[r]

    inside(0)

    pair.wait_recv()
    first_core = c == 0
    for n in range(4):
        own, far = whole_send[4 * c + n], pair_recv[n]
        own_through, far_through = from_parts(own[128:136]), from_parts(far[128:136])
        own_state, far_state = own[0:128].astype(F32), far[0:128].astype(F32)
        earlier = jnp.where(first_core, own_state, far_state)
        later = jnp.where(first_core, far_state, own_state)
        total = jnp.where(first_core, far_through, own_through) * earlier + later
        tail = in_parts(own_through * far_through)
        for r in range(4):
            chunk_send[n * 4 + r, 0:32, :] = total[r * 32:(r + 1) * 32].astype(BF16)
            chunk_send[n * 4 + r, 32:40, :] = tail

    @pl.loop(1, 16)
    def _(i):
        remote(chunk_send.at[(chip + i) % 16], chunk_recv.at[chip], chunk_ss, chunk_rs, same_core(i)).start()

    chunk_recv[chip] = chunk_send[chip]

    slice_send(2)
    inside(1)
    inside(2)
    for m in range(DIRECT_PIECES):
        for j in (0, 1):
            direct_copy(j, m).start()

    relay(0, 0)
    relay(0, 1)

    arrived = chunk_recv.at[pl.ds(0, 15)]
    chunk_all = remote(arrived, arrived, chunk_ss, chunk_rs, other)
    chunk_all.wait_recv()

    state = jnp.zeros((32, 128), F32)
    for t in range(16):
        inc_send[t] = state.astype(BF16)
        state = from_parts(chunk_recv[t, 32:40, :]) * state + chunk_recv[t, 0:32, :].astype(F32)

    @pl.loop(1, 16)
    def _(i):
        remote(inc_send.at[(chip + i) % 16], inc_recv.at[chip], inc_ss, inc_rs, same_core(i)).start()

    inc_recv[chip] = inc_send[chip]

    relay(1, 0)
    relay(1, 1)
    inside(3)
    relay(0, 2)

    returned = inc_recv.at[pl.ds(0, 15)]
    inc_all = remote(returned, returned, inc_ss, inc_rs, other)
    inc_all.wait_recv()
    for n in range(4):
        own, far = whole_send[4 * c + n], pair_recv[n]
        first_state = jnp.where(first_core, own[0:128].astype(F32), far[0:128].astype(F32))
        first_through = jnp.where(first_core, from_parts(own[128:136]), from_parts(far[128:136]))
        reaching = inc_recv[n * 4:(n + 1) * 4].reshape(STATE, 128)
        second = (first_through * reaching.astype(F32) + first_state).astype(BF16)
        incoming[4 * c + n] = jnp.where(first_core, reaching.astype(F32), second.astype(F32)).astype(BF16)
        pair_out[n] = jnp.where(first_core, second.astype(F32), reaching.astype(F32)).astype(BF16)
    handed = remote(pair_out, incoming.at[pl.ds(4 * c, 4)], last_ss, last_rs, other)
    handed.start()
    relay(2, 0)
    relay(2, 1)
    handed.wait_recv()
    copies_in[5].wait()
    copies_in[6].wait()

    def finish(b, put):
        rows = pl.ds(pl.multiple_of(b * SPAN, SPAN), SPAN)
        query = cmat[rows, :]

        def part(q, squares):
            lanes = pl.ds(pl.multiple_of(q * 128, 128), 128)
            state = (starts[b, q] + reach[b, q, 0:1, :] * incoming[q].astype(F32)).astype(BF16)
            inter = jnp.dot(query, state, preferred_element_type=F32)
            value = local[rows, lanes] + grow[rows, lanes] * inter
            v = gate[rows, lanes].astype(F32)
            gated = value * (v / (1.0 + jnp.exp(-v)))
            put(lanes, (gated * gain[:, lanes]).astype(BF16))
            return squares + gated * gated

        squares = lax.fori_loop(0, 8, part, jnp.zeros((SPAN, 128), F32))
        total = jnp.broadcast_to(jnp.sum(squares, axis=1, keepdims=True), (SPAN, 128)).T[0:16, :]
        high = total.astype(BF16).astype(F32)
        return jnp.where(iota((16, SPAN), 0) == 0, high, total - high).astype(BF16)

    def hid_copy(j):
        there = hid.at[h, pl.ds(pl.multiple_of(c * SPAN, SPAN), SPAN), :]
        return remote(hid_send.at[j], there, hid_ss.at[j], hid_rs.at[arrives_as[j]], (s, planes[j]))

    def far_copy(j):
        return remote(hid_send.at[j], hid_far.at[j], far_ss.at[j], far_rs.at[j], other)

    def product_copy(j):
        there = product_recv.at[arrives_as[j]]
        return remote(product_send.at[j], there, product_ss.at[j], product_rs.at[arrives_as[j]], (s, planes[j]))

    def product_all(j):
        part = product_recv.at[j]
        return remote(part, part, product_ss.at[j], product_rs.at[j], (s, planes[j]))


    there, here = (pl.ds(pl.multiple_of(core * SPAN, SPAN), SPAN) for core in (1 - c, c))

    def sum_copy(j):
        return remote(sums_send.at[j], sums.at[c, h], sum_ss, sum_rs, (s, planes[j]))

    for j in (2, 0, 1):
        def put(lanes, value, j=j):
            hid_send[j, :, lanes] = value

        sums_send[j] = finish(planes[j], put)
        hid_copy(j).start()
        sum_copy(j).start()
        if j < 2:
            far_copy(j).start()
        if j == 2:
            relay(1, 2)

    relay(3, 0)

    def put_own(lanes, value):
        hid[h, pl.ds(pl.multiple_of(c * SPAN, SPAN), SPAN), lanes] = value

    sums[c, h] = finish(h, put_own)

    def forward(n, plane):
        part = hid.at[plane, pl.ds(pl.multiple_of(c * SPAN, SPAN), SPAN), :]
        return remote(part, part, fwd_ss.at[n], fwd_rs.at[n], other)

    forward(3, h).start()

    for j in (0, 1):
        far_copy(j).wait_recv()
        for rows, value in ((here, hid_send), (there, hid_far)):
            product_send[j, rows, :] = jnp.dot(value[j], weight[h, :, PRODUCT], preferred_element_type=F32).astype(BF16)
        product_copy(j).start()

    relay(2, 2)
    relay(3, 1)

    forward(3, h).wait_recv()

    @pl.loop(0, 8)
    def _(n):
        lanes = pl.ds(pl.multiple_of(n * 256, 256), 256)
        acc[:, lanes] = jnp.dot(hid[h], weight[h, :, lanes], preferred_element_type=F32)

    def wait_hid(j):
        part = hid.at[planes[j], pl.ds(pl.multiple_of(c * SPAN, SPAN), SPAN), :]
        remote(part, part, hid_ss.at[j], hid_rs.at[j], (s, planes[j])).wait_recv()
        forward(j, planes[j]).start()

    def depth_of(k, last):
        first = (mine[k] // 8) * 512
        if last:
            first = 512 - first
        return pl.ds(pl.multiple_of(first, 512), 512)

    def multiply(j, last):
        for k in range(4):
            depth = depth_of(k, last)
            column, width = COLOURS[j][k]
            lanes = slice(column, column + width)
            acc[:, lanes] += jnp.dot(hid[planes[j], :, depth], weight[planes[j], depth, lanes], preferred_element_type=F32)

    wait_hid(2)
    forward(2, planes[2]).wait_recv()
    relay(3, 2)
    multiply(2, False)
    for j in (0, 1):
        wait_hid(j)
    totals = sums.at[c, pl.ds(0, 3)]
    remote(totals, totals, sum_ss, sum_rs, other).wait_recv()
    forward_sums = remote(sums.at[c], sums.at[c], fsum_ss, fsum_rs, other)
    forward_sums.start()
    for j in (0, 1):
        forward(j, planes[j]).wait_recv()
        multiply(j, False)

    forward_sums.wait_recv()

    def scales(core):
        total = jnp.zeros((16, SPAN), F32)
        for n in range(4):
            total = total + sums[core, n].astype(F32)
        both = lax.rsqrt((total[0:1] + total[1:2]) / INNER + 1e-05)
        return jnp.broadcast_to(both, (128, SPAN)).T

    scale_there, scale_here = scales(1 - c), scales(c)

    for j in (0, 1):
        step_all(3, j).wait_recv()
        multiply(j, True)
    for j in (0, 1):
        for m in range(DIRECT_PIECES):
            direct_wait(j, m)
        acc[:, DIRECT] += jnp.dot(hid[planes[j]], weight[planes[j], :, DIRECT], preferred_element_type=F32)
    def finish_part(n, colours):
        offset, width = LAST[n]
        spans = {k: slice(k * 512 + offset, k * 512 + offset + width) for k in colours}
        columns = {k: pl.ds(pl.multiple_of(base + k * 512 + offset, 128), width) for k in colours}

        def ended(rows, scale):
            scale = jnp.concatenate([scale] * (width // 128), axis=1)
            terms = {}
            for k in colours:
                depth = depth_of(k, True)
                terms[k] = jnp.dot(hid[planes[2], rows, depth], weight[planes[2], depth, spans[k]], preferred_element_type=F32)
            return {k: ((acc[rows, spans[k]] + terms[k]) * scale).astype(BF16) for k in colours}

        for k, value in ended(there, scale_there).items():
            done[:, spans[k]] = value
        for k in colours:
            remote(done.at[:, spans[k]], out.at[:, columns[k]], out_ss, out_rs, other).start()
        for k, value in ended(here, scale_here).items():
            out[:, columns[k]] = value

    early, late = (0, 1, 2), (3,)
    for n in (0, 1):
        step_all(3, 2, n).wait_recv()
        finish_part(n, early)
    for j in (0, 1):
        product_all(j).wait_recv()
    acc[:, PRODUCT] += product_recv[0].astype(F32) + product_recv[1].astype(F32)
    for n in (0, 1):
        finish_part(n, late)
    step_all(3, 2, 2).wait_recv()
    finish_part(2, early + late)

    for j in (0, 1, 2):
        slice_all(j).wait_send()
        for t in range(4):
            for n in range(step_parts(t, j)):
                step_all(t, j, n).wait_send()
        hid_copy(j).wait_send()
        forward(j, planes[j]).wait_send()
    totals_sent = remote(sums_send, sums_send, sum_ss, sum_rs, other)
    totals_sent.wait_send()
    for j in (0, 1):
        far_copy(j).wait_send()
        product_copy(j).wait_send()
        for m in range(DIRECT_PIECES):
            direct_copy(j, m).wait_send()
    forward(3, h).wait_send()
    forward_sums.wait_send()
    pair.wait_send()
    chunk_all.wait_send()
    inc_all.wait_send()
    handed.wait_send()
    whole = remote(done, done, out_ss, out_rs, other)
    whole.wait_send()
    whole.wait_recv()


def local(xs, gate_branch, bmat, cmat, dt_code, resets, decay_rate, skip, norm_gain, out_weight):
    vmem = pl.BlockSpec(memory_space=pltpu.VMEM)
    hbm = pl.BlockSpec(memory_space=pl.ANY)
    dma = pltpu.SemaphoreType.DMA
    V = pltpu.VMEM
    return pl.pallas_call(
        kernel,
        out_shape=pltpu.VMEM((256, 4096), BF16),
        in_specs=[hbm] * 10,
        out_specs=vmem,
        scratch_shapes=[
            pltpu.SMEM((16,), F32),
            pltpu.SMEM((16,), F32),
            V((1024, 1024), BF16),
            V((1024, 1024), BF16),
            V((1024, 128), BF16),
            V((1024, 128), BF16),
            V((16, 1024), jnp.int32),
            V((1, 1024), jnp.int32),
            V((1, 1024), F32),
            V((4, 1024, 2048), BF16),
            V((4, 512, 1024), BF16),
            V((3, 256, 1024), BF16),
            V((2, 256, 1024), BF16),
            V((2, 512, 512), BF16),
            V((2, 512, 512), BF16),
            V((2, 4, 16, 256), BF16),
            V((3, 16, 256), BF16),
            V((512, 2048), F32),
            V((256, 2048), BF16),
            V((256, 256), BF16),
            V((4, 256, 128), F32),
            V((4, 256, 256), BF16),
            V((4, 128, 256), BF16),
            V((4, 16, 256), F32),
            V((4, 8, 256), F32),
            V((1024, 1024), F32),
            V((4, 8, 128, 128), F32),
            V((4, 8, 8, 128), F32),
            V((8, 136, 128), BF16),
            V((4, 136, 128), BF16),
            V((16, 40, 128), BF16),
            V((16, 40, 128), BF16),
            V((16, 32, 128), BF16),
            V((16, 32, 128), BF16),
            V((4, 128, 128), BF16),
            V((8, 128, 128), BF16),
            V((256, 256), F32),
            V((1024, 1024), F32),
            dma((9,)), dma, dma((3,)), dma((3,)),
            dma((2, DIRECT_PIECES)), dma((2, DIRECT_PIECES)), dma((2,)), dma((2,)), dma((2,)), dma((2,)), dma((4, 5)), dma((4, 5)),
            dma, dma, dma, dma, dma, dma, dma, dma,
            dma((3,)), dma((3,)), dma, dma, dma((4,)), dma((4,)), dma, dma,
            dma, dma,
        ],
        compiler_params=pltpu.CompilerParams(
            collective_id=0, has_side_effects=True, vmem_limit_bytes=58 * 1024 * 1024
        ),
    )(
        xs, gate_branch, bmat, cmat, dt_code, resets.reshape(1, 1024), norm_gain.reshape(1, 1024), out_weight,
        decay_rate, skip,
    )


def solution(mesh):
    in_specs = (
        P("seq", "head"),
        P("seq", "head"),
        P("seq", None),
        P("seq", None),
        P("head", "seq"),
        P("seq"),
        P("head"),
        P("head"),
        P("head"),
        P("head", None),
    )
    out_specs = P(("seq", "head"), None)
    return jax.shard_map(local, mesh=mesh, in_specs=in_specs, out_specs=out_specs, check_vma=False)
```
